32 devices in a mesh: blk: 4 (over y, core), grp: 8 (over z, x).
Axes of the slice: x: 2, y: 2, z: 4, core: 2. Of those that a mesh axis runs over, the one named last changes fastest.
Arguments:
- gas_state: bfloat16 [16, 32, 32768], P(None, None, ('grp', 'blk')), may hold values from -6 to 6
- cos_zenith: bfloat16 [32768], P(('grp', 'blk')), may hold values from 0.049804688 to 1
- daylit: int32 [32768], P(('grp', 'blk')), may hold values from 0 to 1
- fine_area: float32 [131072], P(('grp', 'blk')), may hold values from 0.25 to 4
- fine_albedo: float32 [2, 131072], P(None, ('grp', 'blk')), may hold values from 0.05 to 0.85
- parent_of: int32 [131072], P(('grp', 'blk')), may hold values from 0 to 4095, as said below
- optics_weight: bfloat16 [64, 16], replicated, may hold values from -1.5 to 1.5
- solar_weight: float32 [32], replicated, may hold values from 0.01 to 0.1
- neighbours: int32 [3, 32768], P(None, ('grp', 'blk')), may hold values from 0 to 32767, as said below
- side_weight: float32 [3, 32768], P(None, ('grp', 'blk')), may hold values from 0.05 to 0.3
Outputs:
- fluxes: float32 [2, 33, 32768], P(None, None, ('grp', 'blk'))
The draws below stay inside these ranges and needn't reach their ends.
Inputs may be any that keep to these rules, and one draw needn't show every extreme that they name: `parent_of`: the fine cells of one index of grp have their parents among that index's columns, numbered from 0 within it; each column has exactly 4 fine cells, and the 128 fine cells of an aligned block share 128 // 4 consecutive columns. `neighbours`: every neighbour lies within 128 columns of its column and among the columns of the same index of grp; a neighbour may be the column itself.
All inputs are finite; a program needn't handle non-finite values.
Results may differ from the reference program's by a relative error of at most 0.0003.
Values may be sent and summed in bfloat16 or wider, within the bound.
A program may use at most 64 MiB of HBM per device.

```python
import math
import jax
import jax.numpy as jnp
from jax import lax

G = 32
F = 16
LEV = 32
COLS_DEV = 1024
CB = 128
KIDS = 4
FB = 128
REACH = 128
GROUP_COLS = 4096
COLUMNS = 32768
FINE = 131072
N_BLK = 4
N_GRP = 8


def draw_daylit(key, part):
    devices = N_GRP * N_BLK
    nblocks = COLS_DEV // CB
    key_one, key_two, key_three = jax.random.split(jax.random.fold_in(key, 11), 3)
    blk_place = jnp.arange(devices, dtype=jnp.int32) % N_BLK
    trend = blk_place * nblocks // max(N_BLK - 1, 1)
    jitter = jax.random.randint(key_one, (devices,), -(nblocks // 2), nblocks // 2 + 1)
    lit_blocks = jnp.clip(trend + jitter, 0, nblocks)
    scores = jax.random.randint(key_two, (devices, nblocks), 0, 1 << 16) * nblocks + jnp.arange(nblocks, dtype=jnp.int32)[None, :]
    ordering = jnp.argsort(scores, axis=1)
    ranking = jnp.argsort(ordering, axis=1)
    partial_len = jax.random.randint(key_three, (devices, 1, 1), 1, CB)
    inside = jnp.arange(CB, dtype=jnp.int32)[None, None, :]
    fully = ranking[:, :, None] < lit_blocks[:, None, None]
    border = (ranking[:, :, None] == lit_blocks[:, None, None]) & (inside < partial_len)
    return (fully | border).astype(jnp.int32).reshape(COLUMNS)


def draw_parent_of(key, part):
    per_span = FB // KIDS
    spans = GROUP_COLS // per_span
    key_one, key_two = jax.random.split(jax.random.fold_in(key, 23))
    scores = jax.random.randint(key_one, (N_GRP, spans), 0, 1 << 12) * spans + jnp.arange(spans, dtype=jnp.int32)[None, :]
    span_order = jnp.argsort(scores, axis=1).astype(jnp.int32)
    inner_scores = jax.random.randint(key_two, (N_GRP, spans, FB), 0, 1 << 16) * FB + jnp.arange(FB, dtype=jnp.int32)[None, None, :]
    inner = jnp.argsort(inner_scores, axis=2).astype(jnp.int32) % per_span
    parent = span_order[:, :, None] * per_span + inner
    return parent.reshape(FINE).astype(jnp.int32)


def draw_neighbours(key, part):
    column = jnp.arange(COLUMNS, dtype=jnp.int32)
    lower = column // GROUP_COLS * GROUP_COLS
    offsets = jax.random.randint(jax.random.fold_in(key, 37), (3, COLUMNS), -REACH, REACH + 1)
    return jnp.clip(column[None, :] + offsets, lower[None, :], lower[None, :] + GROUP_COLS - 1).astype(jnp.int32)


def block_scale(key, dims, shards, low, top_value):
    def one(axis_at, blocks):
        draws = jax.random.uniform(jax.random.fold_in(jax.random.fold_in(key, 6), axis_at), (blocks,), jnp.float32, low / len(shards), top_value / len(shards))
        return jnp.repeat(jnp.exp(draws), dims[axis_at] // blocks).reshape((-1,) + (1,) * (len(dims) - axis_at - 1))

    gain = one(*shards[0])
    for cut in shards[1:]:
        gain = gain * one(*cut)
    return gain


def bell_draw(own_key, extent, scale, bound, shards=(), kind=jnp.bfloat16):
    values = scale * jax.random.normal(own_key, extent, jnp.float32)
    if shards:
        values = values * block_scale(own_key, extent, shards, -0.22, 0.18)
    return jnp.clip(values, -bound, bound).astype(kind)


def setup_inputs(seed: int = 0) -> dict:
    seeds = jax.random.split(jax.random.key(seed), 11)
    gas_state = bell_draw(seeds[0], (F, LEV, COLUMNS), 1.0, 6.0, ((2, 32),))
    cos_zenith = jnp.clip(0.049804688 + 0.9501953 * jax.random.uniform(seeds[1], (COLUMNS,), jnp.float32) ** block_scale(seeds[1], (COLUMNS,), ((0, 32),), -0.2, 0.2), 0.049804688, 1.0).astype(jnp.bfloat16)
    daylit = draw_daylit(jax.random.fold_in(seeds[10], 71), 0)
    fine_area = jnp.clip(jnp.exp(math.log(4.0) - 2.7725887 * jax.random.uniform(seeds[3], (FINE,), jnp.float32) ** block_scale(seeds[3], (FINE,), ((0, 32),), -0.2, 0.2)), 0.25, 4.0)
    fine_albedo = jnp.clip(0.05 + 0.8 * jax.random.uniform(seeds[4], (2, FINE), jnp.float32) ** block_scale(seeds[4], (2, FINE), ((1, 32),), -0.2, 0.2), 0.05, 0.85)
    parent_of = draw_parent_of(jax.random.fold_in(seeds[10], 71), 0)
    optics_weight = bell_draw(seeds[6], (2 * G, F), F ** -0.5, 1.5)
    solar_weight = jnp.clip(jnp.exp(jax.random.uniform(seeds[7], (G,), jnp.float32, math.log(0.01), math.log(0.1))), 0.01, 0.1)
    neighbours = draw_neighbours(jax.random.fold_in(seeds[10], 71), 0)
    side_weight = jnp.clip(0.05 + 0.25 * jax.random.uniform(seeds[9], (3, COLUMNS), jnp.float32) ** block_scale(seeds[9], (3, COLUMNS), ((1, 32),), -0.2, 0.2), 0.05, 0.3)
    return dict(gas_state=gas_state, cos_zenith=cos_zenith, daylit=daylit, fine_area=fine_area, fine_albedo=fine_albedo, parent_of=parent_of, optics_weight=optics_weight, solar_weight=solar_weight, neighbours=neighbours, side_weight=side_weight)


ASYM = 0.8
TAU_SCALE = 0.08
SSA_MAX = 0.98

def column_fluxes(optics_mix, cosine_col, albedo_direct, albedo_diffuse, lit_flag, solar_weight):
    gpoints = solar_weight.shape[0]
    width = cosine_col.shape[0]
    optical_depth = TAU_SCALE * jax.nn.softplus(optics_mix[:, :gpoints])
    single_albedo = SSA_MAX * jax.nn.sigmoid(optics_mix[:, gpoints:])
    slant = cosine_col[None, None, :]
    direct_share = jnp.exp(-optical_depth / slant)
    gamma_one = 2.0 - single_albedo * (1.25 + 0.75 * ASYM)
    gamma_two = 0.75 * single_albedo * (1.0 - ASYM)
    eigen_rate = jnp.sqrt((gamma_one - gamma_two) * (gamma_one + gamma_two))
    damping = jnp.exp(-eigen_rate * optical_depth)
    damped_sq = damping * damping
    divisor = eigen_rate + gamma_one + (eigen_rate - gamma_one) * damped_sq
    reflect = gamma_two * (1.0 - damped_sq) / divisor
    transmit = 2.0 * eigen_rate * damping / divisor
    back_share = 0.5 * (1.0 - ASYM * slant)
    scattered = single_albedo * (1.0 - direct_share)
    rising = scattered * back_share
    falling = scattered - rising
    top_flux = solar_weight[:, None] * cosine_col[None, :]
    direct = top_flux[None] * jnp.concatenate([jnp.ones_like(top_flux)[None], jnp.cumprod(direct_share, axis=0)], axis=0)

    def ascend(carry, layer):
        albedo, source = carry
        inverse = 1.0 / (1.0 - albedo * layer[0])
        new_albedo = layer[0] + layer[1] * layer[1] * albedo * inverse
        new_source = layer[2] * layer[4] + layer[1] * (source + albedo * layer[3] * layer[4]) * inverse
        return ((new_albedo, new_source), (albedo, source, inverse))
    ground = (jnp.broadcast_to(albedo_diffuse[None, :], top_flux.shape), albedo_direct[None, :] * direct[-1])
    (top_albedo, source_top), below = lax.scan(ascend, ground, (reflect, transmit, rising, falling, direct[:-1]), reverse=True)

    def descend(diffuse, layer):
        updated = (layer[1] * diffuse + layer[0] * layer[6] + layer[3] * layer[4]) * layer[7]
        return (updated, (updated, layer[5] * updated + layer[6]))
    last_diffuse, (diffuse_down, diffuse_up) = lax.scan(descend, jnp.zeros_like(top_flux), (reflect, transmit, rising, falling, direct[:-1], below[0], below[1], below[2]))
    first_row = jnp.zeros((1, width), jnp.float32)
    downward = lax.optimization_barrier(jnp.sum(direct, axis=1)) + jnp.concatenate([first_row, lax.optimization_barrier(jnp.sum(diffuse_down, axis=1))], axis=0)
    upward = jnp.concatenate([lax.optimization_barrier(jnp.sum(source_top, axis=0))[None], lax.optimization_barrier(jnp.sum(diffuse_up, axis=1))], axis=0)
    return jnp.stack([downward, upward]) * lit_flag[None, None, :]

def reference(gas_state, cos_zenith, daylit, fine_area, fine_albedo, parent_of, optics_weight, solar_weight, neighbours, side_weight):
    weights = jnp.stack([fine_area, fine_area * fine_albedo[0], fine_area * fine_albedo[1]])
    fine_group = (jnp.arange(FINE, dtype=jnp.int32) // (KIDS * GROUP_COLS)).astype(jnp.int32)
    parent_global = (parent_of + fine_group * GROUP_COLS).astype(jnp.int32)
    totals = jax.vmap(lambda values: jax.ops.segment_sum(values, parent_global, num_segments=COLUMNS))(weights)
    albedo = (totals[1:] / totals[0]).astype(jnp.bfloat16).astype(jnp.float32)
    cosine_all = cos_zenith.astype(jnp.float32)
    lit_all = daylit.astype(jnp.float32)
    matrix = optics_weight.astype(jnp.float32)
    nblocks = COLUMNS // COLS_DEV

    def one_block(number):
        begin_at = (number * COLS_DEV).astype(jnp.int32)
        inputs = lax.dynamic_slice_in_dim(gas_state, begin_at, COLS_DEV, 2).astype(jnp.float32)
        optics_mix = jnp.einsum('gf,fln->lgn', matrix, inputs, precision=lax.Precision.HIGHEST)
        cosine_col = lax.dynamic_slice_in_dim(cosine_all, begin_at, COLS_DEV, 0)
        albedo_cols = lax.dynamic_slice_in_dim(albedo, begin_at, COLS_DEV, 1)
        lit_cols = lax.dynamic_slice_in_dim(lit_all, begin_at, COLS_DEV, 0)
        return column_fluxes(optics_mix, cosine_col, albedo_cols[0], albedo_cols[1], lit_cols, solar_weight)
    stacked = lax.map(one_block, jnp.arange(nblocks, dtype=jnp.int32))
    column_flux = jnp.moveaxis(stacked, 0, 2).reshape(2, LEV + 1, COLUMNS)
    result = column_flux
    for index_k in range(3):
        beside = jnp.take(column_flux, neighbours[index_k], axis=2)
        result = result + side_weight[index_k][None, None, :] * (beside - column_flux)
    return result
```

```python
import functools
import math

import jax
import jax.numpy as jnp
from jax import lax
from jax.experimental import pallas as pl
from jax.experimental.pallas import tpu as pltpu
from jax.sharding import PartitionSpec as P

CB = 128
FB = 128
ASYM = 0.8
TAU_SCALE = 0.08
SSA_MAX = 0.98
LOG2E = math.log2(math.e)
CHUNK = 8
VMEM = pltpu.VMEM
GROUND = 2.0 / SSA_MAX - 1.0
DEPTH = 0.5 * TAU_SCALE * math.log(2.0) * SSA_MAX


def round_up(value, multiple):
    return -(-value // multiple) * multiple


def local_albedo(area_ref, albedo_ref, parent_ref, span):
    blocks = area_ref.shape[0]
    area = area_ref[...]
    rows = [
        jnp.concatenate([albedo_ref[s : s + 1, b * FB : (b + 1) * FB] for b in range(blocks)], axis=0)
        for s in range(2)
    ]
    weights = jnp.transpose(jnp.concatenate([area, area * rows[0], area * rows[1]], axis=0))
    parent = jnp.transpose(jnp.concatenate([parent_ref[...]] * 3, axis=0))
    inside = parent & (span - 1)
    totals = jnp.concatenate(
        [jnp.sum(jnp.where(inside == j, weights, 0.0), axis=0, keepdims=True) for j in range(span)], axis=0
    )
    share = totals[:, :blocks]
    first = (totals[:, blocks : 2 * blocks] / share).astype(jnp.bfloat16).astype(jnp.float32)
    second = (totals[:, 2 * blocks :] / share).astype(jnp.bfloat16).astype(jnp.float32)
    number = (parent[0:1, :blocks] // span).astype(jnp.float32)
    return first, second, number


def pick_albedo(pieces, start_span, span, blocks, ncb):
    per = CB // span
    table = jnp.concatenate(
        [jnp.concatenate([p[0:span, s * blocks : (s + 1) * blocks] for p in pieces], axis=1) for s in range(2)],
        axis=0,
    ).astype(jnp.bfloat16)
    number = jnp.concatenate([p[span : span + 1, 0:blocks] for p in pieces], axis=1).astype(jnp.int32)
    total = number.shape[1]
    row = lax.broadcasted_iota(jnp.int32, (ncb, total), 0) * per + start_span
    parts = []
    for m in range(per):
        chosen = (number == row + m).astype(jnp.float32).astype(jnp.bfloat16)
        parts.append(
            lax.dot_general(chosen, table, (((1,), (1,)), ((), ())), preferred_element_type=jnp.float32)
        )
    direct = jnp.concatenate([p[:, 0:span] for p in parts], axis=1)
    diffuse = jnp.concatenate([p[:, span : 2 * span] for p in parts], axis=1)
    return direct, diffuse


def expand_weight(weight_ref, big_ref):
    feats, rows = weight_ref.shape
    wide = big_ref.shape[1]
    source = lax.broadcasted_iota(jnp.int32, (feats, wide), 0)
    column = lax.broadcasted_iota(jnp.int32, (feats, wide), 1)
    spread = (column % (wide // 2) // CHUNK == source).astype(jnp.float32).astype(jnp.bfloat16)
    repeated = lax.dot_general(
        weight_ref[...], spread, (((0,), (0,)), ((), ())), preferred_element_type=jnp.float32
    )
    row = lax.broadcasted_iota(jnp.int32, (rows, wide), 0)
    place = lax.broadcasted_iota(jnp.int32, (rows, wide), 1)
    scaled = jnp.where(row < rows // 2, LOG2E * repeated, 0.5 * repeated)
    high = scaled.astype(jnp.bfloat16).astype(jnp.float32)
    scaled = jnp.where(place < wide // 2, high, scaled - high)
    level = place % CHUNK
    for l in range(CHUNK):
        big_ref[l * rows : (l + 1) * rows, :] = jnp.where(level == l, scaled, 0.0).astype(jnp.bfloat16)


def product(block, first, gas_ref, big_ref, mix_ref):
    feats = gas_ref.shape[0]
    cols = pl.ds(pl.multiple_of(block * CB, CB), CB)
    inputs = gas_ref[:, first : first + CHUNK, cols].reshape(feats * CHUNK, CB)
    mix_ref[...] = jnp.dot(
        big_ref[...], jnp.concatenate([inputs, inputs], axis=0), preferred_element_type=jnp.float32
    )


def layer(mix, rate, coef_ref, place):
    gpoints = mix.shape[0] // 2
    x = mix[:gpoints]
    soft = jnp.maximum(x, lax.log2(1.0 + jnp.exp2(jnp.minimum(x, 100.0))))
    u = jnp.tanh(mix[gpoints:])
    wide = 1.0 + u
    less = GROUND - u
    gap = 0.15 * wide
    more = less + gap
    square = less * more
    inverse = lax.rsqrt(square)
    bend = jnp.tanh(((square * inverse) * soft) * DEPTH)
    slope = bend * inverse
    total = (less + more) * slope
    bend2 = bend * bend
    plus = 1.0 + bend2
    coef_ref[0, place] = jnp.exp2(soft * rate)
    coef_ref[1, place] = wide
    coef_ref[2, place] = gap * slope
    coef_ref[3, place] = plus + total
    coef_ref[4, place] = plus - total
    coef_ref[5, place] = 1.0 - bend2


def recur(coef_ref, place, level, state_ref, back, fall, carry):
    direct, big_b, big_q = carry
    r, d, dd, t2 = [coef_ref[i, place] for i in range(2, 6)]
    below = direct * coef_ref[0, place]
    scattered = coef_ref[1, place] * (direct - below)
    rising = scattered * back
    falling = scattered * fall
    state_ref[2, level] = big_b
    state_ref[3, level] = big_q + direct
    z = 1.0 / (d - r * big_b)
    h = (big_q + big_b * rising) * z
    state_ref[0, level] = t2 * z
    state_ref[1, level] = r * h + rising
    return below, (r + dd * big_b) * z, t2 * h + falling


def fold(parts):
    place = lax.broadcasted_iota(jnp.int32, parts[0].shape, 0)
    distance = 1
    while len(parts) > 1:
        even = (place & distance) == 0
        parts = [
            jnp.where(even, p, q) + pltpu.roll(jnp.where(even, q, p), 8 - distance, 0)
            for p, q in zip(parts[0::2], parts[1::2])
        ]
        distance *= 2
    rest = parts[0]
    while distance < 8:
        rest = rest + pltpu.roll(rest, 8 - distance, 0)
        distance *= 2
    return rest


def gather_g(value):
    parts = [value[i : i + 8] for i in range(0, value.shape[0], 8)]
    while len(parts) > 1:
        parts = [p + q for p, q in zip(parts[0::2], parts[1::2])]
    return parts[0]


class Ascent:
    def __init__(self, cb, albedo_ref, lit_ref, state_ref, end_ref, flux_ref):
        lev = state_ref.shape[1]
        self.state_ref, self.flux_ref = state_ref, flux_ref
        self.lit = lit_ref[pl.ds(cb, 1), :]
        direct, big_b, big_q = end_ref[0], end_ref[1], end_ref[2]
        direct_albedo = albedo_ref[0, pl.ds(cb, 1), :]
        diffuse_albedo = albedo_ref[1, pl.ds(cb, 1), :]
        self.up = (diffuse_albedo * big_q + direct_albedo * direct) / (1.0 - diffuse_albedo * big_b)
        last = fold([gather_g(big_b * self.up + big_q + direct), gather_g(self.up)])
        flux_ref[2 * lev : 2 * lev + 8, :] = last * self.lit
        self.parts = []

    def level(self, level):
        state_ref = self.state_ref
        self.up = state_ref[0, level] * self.up + state_ref[1, level]
        down = state_ref[2, level] * self.up + state_ref[3, level]
        self.parts = [gather_g(down), gather_g(self.up)] + self.parts
        if level % 4 == 0:
            self.flux_ref[2 * level : 2 * level + 8, :] = fold(self.parts) * self.lit
            self.parts = []


def solar_column(solar_ref):
    row = solar_ref[...]
    n = row.shape[1]
    diagonal = lax.broadcasted_iota(jnp.int32, (n, n), 0) == lax.broadcasted_iota(jnp.int32, (n, n), 1)
    return jnp.sum(jnp.where(diagonal, row, 0.0), axis=1, keepdims=True)


def flux_kernel(
    n, span, gas_hbm, cos_ref, lit_ref, weight_ref, solar_ref, area_ref, fine_albedo_ref, parent_ref,
    flux_ref, big_ref, state_ref, end_ref, albedo_ref, cosf_ref, litf_ref, mine_ref, pieces_ref,
    edge_ref, halo_ref, mix_ref, early_ref, late_ref, gas_ref, send_sem, recv_sem, edge_send, edge_recv, gas_sem,
):
    ncb = cos_ref.shape[0]
    blocks = area_ref.shape[0]
    lev = gas_ref.shape[1]
    gpoints = solar_ref.shape[1]
    rows = 2 * gpoints
    half = lev // 2
    slots = state_ref.shape[0]
    me = lax.axis_index("blk")
    peers = [lax.rem(me + shift, n) for shift in range(1, n)]
    mesh_id = pl.DeviceIdType.MESH

    load = pltpu.make_async_copy(gas_hbm, gas_ref, gas_sem)
    load.start()
    barrier = pltpu.get_barrier_semaphore()
    for peer in peers:
        pl.semaphore_signal(barrier, inc=1, device_id={"blk": peer}, device_id_type=mesh_id)

    first, second, number = local_albedo(area_ref, fine_albedo_ref, parent_ref, span)
    mine_ref[...] = jnp.zeros_like(mine_ref)
    mine_ref[0:span, 0:blocks] = first
    mine_ref[0:span, blocks : 2 * blocks] = second
    mine_ref[span : span + 1, 0:blocks] = number
    expand_weight(weight_ref, big_ref)
    cosf_ref[...] = cos_ref[...].astype(jnp.float32)
    litf_ref[...] = lit_ref[...].astype(jnp.float32)
    solar = solar_column(solar_ref)

    def order(i):
        return jnp.where(i < 2, i * (ncb - 1), i - 1)

    def wide(row):
        return jnp.broadcast_to(row, (gpoints, CB))

    class Prepare:
        def __init__(self, cb, part, coef_ref):
            self.coef_ref = coef_ref
            self.part = part
            self.rate = wide((-TAU_SCALE) / cosf_ref[pl.ds(cb, 1), :])
            for turn in range(half // CHUNK):
                product(cb, part * half + turn * CHUNK, gas_ref, big_ref, mix_ref.at[part, turn])

        def level(self, place):
            turn, i = place // CHUNK, place % CHUNK
            mix = mix_ref[self.part, turn, i * rows : (i + 1) * rows, :]
            layer(mix, self.rate, self.coef_ref, place)

    coefs = (early_ref, late_ref)

    def ascent(i):
        cb = order(i)
        slot = lax.rem(i, slots)
        return Ascent(cb, albedo_ref, litf_ref, state_ref.at[slot], end_ref.at[slot], flux_ref.at[cb + 1])

    def step(i, ahead, ups):
        cb = order(i)
        slot = lax.rem(i, slots)
        mu = cosf_ref[pl.ds(cb, 1), :]
        back = (0.5 * (0.5 * SSA_MAX)) * (1.0 - ASYM * mu)
        fall = wide(0.5 * SSA_MAX - back)
        back = wide(back)
        zero = jnp.zeros((gpoints, CB), jnp.float32)
        carry = (solar * mu, zero, zero)
        ups = [ascent(j) for j in ups]
        for part in range(2):
            next_one = None
            if part == 0:
                next_one = Prepare(cb, 1, late_ref)
            elif ahead:
                next_one = Prepare(order(i + 1), 0, early_ref)
            for place in range(half):
                level = part * half + place
                for up in ups:
                    up.level(lev - 1 - level)
                carry = recur(coefs[part], place, level, state_ref.at[slot], back, fall, carry)
                if next_one is not None:
                    next_one.level(place)
        for j in range(3):
            end_ref[slot, j] = carry[j]

    load.wait()
    begin = Prepare(0, 0, early_ref)
    for place in range(half):
        begin.level(place)

    pl.semaphore_wait(barrier, n - 1)
    sends = []
    for i, peer in enumerate(peers):
        copy = pltpu.make_async_remote_copy(
            src_ref=mine_ref,
            dst_ref=pieces_ref.at[i],
            send_sem=send_sem.at[i],
            recv_sem=recv_sem.at[i],
            device_id={"blk": peer},
            device_id_type=mesh_id,
        )
        copy.start()
        sends.append(copy)

    def first_steps(i, unused):
        step(i, True, [])
        return unused

    lag = slots - 1
    lax.fori_loop(0, lag, first_steps, 0)
    for copy in sends:
        copy.wait()
    start_span = me * (ncb * CB // span)
    pieces = [mine_ref[...]] + [pieces_ref[i] for i in range(n - 1)]
    direct, diffuse = pick_albedo(pieces, start_span, span, blocks, ncb)
    albedo_ref[0] = direct
    albedo_ref[1] = diffuse

    edges = [
        pltpu.make_async_remote_copy(
            src_ref=edge_ref.at[i],
            dst_ref=halo_ref.at[i],
            send_sem=edge_send.at[i],
            recv_sem=edge_recv.at[i],
            device_id={"blk": peer},
            device_id_type=mesh_id,
        )
        for i, peer in ((0, peers[-1]), (1, peers[0]))
    ]

    def middle_steps(i, unused):
        step(i, True, [i - lag])

        @pl.when(i == lag + 1)
        def _():
            edge_ref[0] = flux_ref[1]
            edge_ref[1] = flux_ref[ncb]
            for copy in edges:
                copy.start()

        return unused

    lax.fori_loop(lag, ncb - 1, middle_steps, 0)
    step(ncb - 1, False, range(ncb - 1 - lag, ncb - 1))
    last = ascent(ncb - 1)
    for level in range(lev):
        last.level(lev - 1 - level)
    for copy in edges:
        copy.wait()
    flux_ref[0] = halo_ref[1]
    flux_ref[ncb + 1] = halo_ref[0]


def side_kernel(flux_ref, neighbours_ref, weights_ref, out_ref):
    interfaces, parts, cols = out_ref.shape
    ncb = cols // CB
    rows = flux_ref.shape[1]
    start = (lax.axis_index("grp") * lax.axis_size("blk") + lax.axis_index("blk")) * cols
    for cb in range(ncb):
        own = slice(cb * CB, (cb + 1) * CB)
        picked = neighbours_ref[:, own] - (start + (cb - 1) * CB)
        weights = weights_ref[:, own]
        lanes, blocks, shares = [], [], []
        for k in range(3):
            row = jnp.broadcast_to(picked[k : k + 1], (8, CB))
            lanes.append(row & (CB - 1))
            blocks.append(row // CB)
            shares.append(jnp.broadcast_to(weights[k : k + 1], (8, CB)))
        for r in range(0, rows, 8):
            near = [flux_ref[cb + j, r : r + 8, :] for j in range(3)]
            result = near[1]
            for k in range(3):
                before, here, after = [
                    jnp.take_along_axis(v, lanes[k], axis=1, mode="promise_in_bounds") for v in near
                ]
                beside = jnp.where(blocks[k] == 0, before, jnp.where(blocks[k] == 1, here, after))
                result = result + shares[k] * (beside - near[1])
            top = r // parts
            count = min(8 // parts, interfaces - top)
            out_ref[top : top + count, :, own] = result[: count * parts].reshape(count, parts, CB)


def local(
    gas_state, cos_zenith, daylit, fine_area, fine_albedo, parent_of,
    optics_weight, solar_weight, neighbours, side_weight,
):
    n = lax.axis_size("blk")
    feats, lev, cols = gas_state.shape
    gpoints = solar_weight.shape[0]
    ncb = cols // CB
    blocks = fine_area.shape[0] // FB
    span = cols // blocks
    rows = round_up(2 * (lev + 1), 8)
    half = lev // 2
    slots = 3
    full = pl.BlockSpec(memory_space=VMEM)
    coef = VMEM((6, half, gpoints, CB), jnp.float32)
    fluxes = pl.pallas_call(
        functools.partial(flux_kernel, n, span),
        out_shape=jax.ShapeDtypeStruct((ncb + 2, rows, CB), jnp.float32),
        in_specs=[pl.BlockSpec(memory_space=pltpu.HBM)] + [full] * 7,
        out_specs=full,
        scratch_shapes=[
            VMEM((CHUNK * 2 * gpoints, 2 * CHUNK * feats), jnp.bfloat16),
            VMEM((slots, 4, lev, gpoints, CB), jnp.float32),
            VMEM((slots, 3, gpoints, CB), jnp.float32),
            VMEM((2, ncb, CB), jnp.float32),
            VMEM((ncb, CB), jnp.float32),
            VMEM((ncb, CB), jnp.float32),
            VMEM((span + 8, 128), jnp.float32),
            VMEM((n - 1, span + 8, 128), jnp.float32),
            VMEM((2, rows, CB), jnp.float32),
            VMEM((2, rows, CB), jnp.float32),
            VMEM((2, half // CHUNK, CHUNK * 2 * gpoints, CB), jnp.float32),
            coef,
            coef,
            VMEM((feats, lev, cols), gas_state.dtype),
            pltpu.SemaphoreType.DMA((n - 1,)),
            pltpu.SemaphoreType.DMA((n - 1,)),
            pltpu.SemaphoreType.DMA((2,)),
            pltpu.SemaphoreType.DMA((2,)),
            pltpu.SemaphoreType.DMA,
        ],
        compiler_params=pltpu.CompilerParams(
            collective_id=0, has_side_effects=True, vmem_limit_bytes=24 << 20
        ),
    )(
        gas_state, cos_zenith.reshape(ncb, CB), daylit.reshape(ncb, CB), optics_weight.T,
        solar_weight.reshape(1, gpoints), fine_area.reshape(blocks, FB), fine_albedo,
        parent_of.reshape(blocks, FB),
    )
    result = pl.pallas_call(
        side_kernel,
        out_shape=jax.ShapeDtypeStruct((lev + 1, 2, cols), jnp.float32),
        in_specs=[full] * 3,
        out_specs=full,
        compiler_params=pltpu.CompilerParams(vmem_limit_bytes=8 << 20),
    )(fluxes, neighbours, side_weight)
    return jnp.transpose(result, (1, 0, 2))


def solution(mesh):
    columns = P(("grp", "blk"))
    last = P(None, ("grp", "blk"))
    in_specs = (
        P(None, None, ("grp", "blk")), columns, columns, columns, last, columns, P(), P(), last, last,
    )
    out_specs = P(None, None, ("grp", "blk"))
    return jax.shard_map(local, mesh=mesh, in_specs=in_specs, out_specs=out_specs, check_vma=False)
```

```python
import functools
import math

import jax
import jax.numpy as jnp
from jax import lax
from jax.experimental import pallas as pl
from jax.experimental.pallas import tpu as pltpu
from jax.sharding import PartitionSpec as P

CB = 128
FB = 128
ASYM = 0.8
TAU_SCALE = 0.08
SSA_MAX = 0.98
LOG2E = math.log2(math.e)
CHUNK = 8
VMEM = pltpu.VMEM
GROUND = 2.0 / SSA_MAX - 1.0
DEPTH = 0.5 * TAU_SCALE * math.log(2.0) * SSA_MAX


def round_up(value, multiple):
    return -(-value // multiple) * multiple


def local_albedo(area_ref, albedo_ref, parent_ref, span):
    blocks = area_ref.shape[0]
    area = area_ref[...]
    rows = [
        jnp.concatenate([albedo_ref[s : s + 1, b * FB : (b + 1) * FB] for b in range(blocks)], axis=0)
        for s in range(2)
    ]
    weights = jnp.transpose(jnp.concatenate([area, area * rows[0], area * rows[1]], axis=0))
    parent = jnp.transpose(jnp.concatenate([parent_ref[...]] * 3, axis=0))
    inside = parent & (span - 1)
    totals = jnp.concatenate(
        [jnp.sum(jnp.where(inside == j, weights, 0.0), axis=0, keepdims=True) for j in range(span)], axis=0
    )
    share = totals[:, :blocks]
    first = (totals[:, blocks : 2 * blocks] / share).astype(jnp.bfloat16).astype(jnp.float32)
    second = (totals[:, 2 * blocks :] / share).astype(jnp.bfloat16).astype(jnp.float32)
    number = (parent[0:1, :blocks] // span).astype(jnp.float32)
    return first, second, number


def pick_albedo(pieces, start_span, span, blocks, ncb):
    per = CB // span
    table = jnp.concatenate(
        [jnp.concatenate([p[0:span, s * blocks : (s + 1) * blocks] for p in pieces], axis=1) for s in range(2)],
        axis=0,
    ).astype(jnp.bfloat16)
    number = jnp.concatenate([p[span : span + 1, 0:blocks] for p in pieces], axis=1).astype(jnp.int32)
    total = number.shape[1]
    row = lax.broadcasted_iota(jnp.int32, (ncb, total), 0) * per + start_span
    parts = []
    for m in range(per):
        chosen = (number == row + m).astype(jnp.float32).astype(jnp.bfloat16)
        parts.append(
            lax.dot_general(chosen, table, (((1,), (1,)), ((), ())), preferred_element_type=jnp.float32)
        )
    direct = jnp.concatenate([p[:, 0:span] for p in parts], axis=1)
    diffuse = jnp.concatenate([p[:, span : 2 * span] for p in parts], axis=1)
    return direct, diffuse


def expand_weight(weight_ref, big_ref):
    feats, rows = weight_ref.shape
    wide = big_ref.shape[1]
    source = lax.broadcasted_iota(jnp.int32, (feats, wide), 0)
    column = lax.broadcasted_iota(jnp.int32, (feats, wide), 1)
    spread = (column % (wide // 2) // CHUNK == source).astype(jnp.float32).astype(jnp.bfloat16)
    repeated = lax.dot_general(
        weight_ref[...], spread, (((0,), (0,)), ((), ())), preferred_element_type=jnp.float32
    )
    row = lax.broadcasted_iota(jnp.int32, (rows, wide), 0)
    place = lax.broadcasted_iota(jnp.int32, (rows, wide), 1)
    scaled = jnp.where(row < rows // 2, LOG2E * repeated, 0.5 * repeated)
    high = scaled.astype(jnp.bfloat16).astype(jnp.float32)
    scaled = jnp.where(place < wide // 2, high, scaled - high)
    level = place % CHUNK
    for l in range(CHUNK):
        big_ref[l * rows : (l + 1) * rows, :] = jnp.where(level == l, scaled, 0.0).astype(jnp.bfloat16)


def stage(block, first, gas_ref, inputs_ref):
    feats = gas_ref.shape[0]
    cols = pl.ds(pl.multiple_of(block * CB, CB), CB)
    inputs_ref[...] = jnp.concatenate(
        [
            gas_ref[:, level : level + CHUNK, cols].reshape(feats * CHUNK, CB)
            for level in (first, first + CHUNK)
        ],
        axis=1,
    )


def product(inputs_ref, big_ref, mix_ref):
    inputs = inputs_ref[...]
    mix_ref[...] = jnp.dot(
        big_ref[...], jnp.concatenate([inputs, inputs], axis=0), preferred_element_type=jnp.float32
    )


def layer(mix, rate, coef_ref, place):
    gpoints = mix.shape[0] // 2
    x = mix[:gpoints]
    soft = jnp.maximum(x, lax.log2(1.0 + jnp.exp2(jnp.minimum(x, 100.0))))
    u = jnp.tanh(mix[gpoints:])
    wide = 1.0 + u
    less = GROUND - u
    gap = 0.15 * wide
    more = less + gap
    square = less * more
    inverse = lax.rsqrt(square)
    bend = jnp.tanh(((square * inverse) * soft) * DEPTH)
    slope = bend * inverse
    total = (less + more) * slope
    bend2 = bend * bend
    plus = 1.0 + bend2
    coef_ref[0, place] = jnp.exp2(soft * rate)
    coef_ref[1, place] = wide
    coef_ref[2, place] = gap * slope
    coef_ref[3, place] = plus + total
    coef_ref[4, place] = plus - total
    coef_ref[5, place] = 1.0 - bend2


def recur(coef_ref, place, state_ref, level, back, fall, carry):
    direct, big_b, big_q = carry
    r, d, dd, t2 = [coef_ref[i, place] for i in range(2, 6)]
    below = direct * coef_ref[0, place]
    scattered = coef_ref[1, place] * (direct - below)
    rising = scattered * back
    falling = scattered * fall
    state_ref[2, level] = big_b
    state_ref[3, level] = big_q + direct
    z = 1.0 / (d - r * big_b)
    h = (big_q + big_b * rising) * z
    state_ref[0, level] = t2 * z
    state_ref[1, level] = r * h + rising
    return below, (r + dd * big_b) * z, t2 * h + falling


def fold(parts):
    place = lax.broadcasted_iota(jnp.int32, parts[0].shape, 0)
    distance = 1
    while len(parts) > 1:
        even = (place & distance) == 0
        parts = [
            jnp.where(even, p, q) + pltpu.roll(jnp.where(even, q, p), 8 - distance, 0)
            for p, q in zip(parts[0::2], parts[1::2])
        ]
        distance *= 2
    rest = parts[0]
    while distance < 8:
        rest = rest + pltpu.roll(rest, 8 - distance, 0)
        distance *= 2
    return rest


def gather_g(value):
    parts = [value[i : i + 8] for i in range(0, value.shape[0], 8)]
    while len(parts) > 1:
        parts = [p + q for p, q in zip(parts[0::2], parts[1::2])]
    return parts[0]


class Ascent:
    def __init__(self, albedo, lit, carry, state_ref, rise_ref):
        lev = state_ref.shape[1]
        self.state_ref, self.rise_ref, self.lit = state_ref, rise_ref, lit
        direct, big_b, big_q = carry
        self.up = (albedo[1] * big_q + albedo[0] * direct) / (1.0 - albedo[1] * big_b)
        last = fold([gather_g(big_b * self.up + big_q + direct), gather_g(self.up)])
        rise_ref[2 * lev : 2 * lev + 8, :] = last * lit
        self.parts = []

    def level(self, level):
        state_ref = self.state_ref
        self.up = state_ref[0, level] * self.up + state_ref[1, level]
        down = state_ref[2, level] * self.up + state_ref[3, level]
        self.parts = [gather_g(down), gather_g(self.up)] + self.parts
        if level % 4 == 0:
            self.rise_ref[2 * level : 2 * level + 8, :] = fold(self.parts) * self.lit
            self.parts = []


def solar_column(solar_ref):
    row = solar_ref[...]
    n = row.shape[1]
    diagonal = lax.broadcasted_iota(jnp.int32, (n, n), 0) == lax.broadcasted_iota(jnp.int32, (n, n), 1)
    return jnp.sum(jnp.where(diagonal, row, 0.0), axis=1, keepdims=True)


def flux_kernel(
    n, span, gas_hbm, cos_ref, lit_ref, weight_ref, solar_ref, area_ref, fine_albedo_ref, parent_ref,
    flux_ref, big_ref, state_ref, first_ref, end_ref, albedo_ref, cosf_ref, litf_ref, mine_ref, pieces_ref,
    edge_ref, halo_ref, inputs_ref, mix_ref, next_ref, coef_ref, rise_ref, gas_ref, send_sem, recv_sem, edge_send, edge_recv, gas_sem,
):
    ncb = cos_ref.shape[0]
    blocks = area_ref.shape[0]
    lev = gas_ref.shape[1]
    gpoints = solar_ref.shape[1]
    rows = 2 * gpoints
    me = lax.axis_index("blk")
    peers = [lax.rem(me + shift, n) for shift in range(1, n)]
    mesh_id = pl.DeviceIdType.MESH

    load = pltpu.make_async_copy(gas_hbm, gas_ref, gas_sem)
    load.start()
    barrier = pltpu.get_barrier_semaphore()
    for peer in peers:
        pl.semaphore_signal(barrier, inc=1, device_id={"blk": peer}, device_id_type=mesh_id)

    first, second, number = local_albedo(area_ref, fine_albedo_ref, parent_ref, span)
    mine_ref[...] = jnp.zeros_like(mine_ref)
    mine_ref[0:span, 0:blocks] = first
    mine_ref[0:span, blocks : 2 * blocks] = second
    mine_ref[span : span + 1, 0:blocks] = number
    expand_weight(weight_ref, big_ref)
    cosf_ref[...] = cos_ref[...].astype(jnp.float32)
    litf_ref[...] = lit_ref[...].astype(jnp.float32)
    solar = solar_column(solar_ref)

    def order(i):
        if isinstance(i, int):
            return i * (ncb - 1) if i < 2 else i - 1
        return jnp.where(i < 2, i * (ncb - 1), i - 1)

    def wide(row):
        return jnp.broadcast_to(row, (gpoints, CB))

    def rate_of(cb):
        return wide((-TAU_SCALE) / cosf_ref[pl.ds(cb, 1), :])

    def stage_pair(cb, pair):
        stage(cb, 2 * pair * CHUNK, gas_ref, inputs_ref.at[pair])

    def multiply(cb, target_ref):
        for pair in range(2):
            stage_pair(cb, pair)
            product(inputs_ref.at[pair], big_ref, target_ref.at[pair])

    class Prepare:
        def __init__(self, rate):
            self.rate, self.done = rate, 0

        def until(self, count):
            for level in range(self.done, int(count)):
                chunk, i = level // CHUNK, level % CHUNK
                left = chunk % 2 * CB
                mix = mix_ref[chunk // 2, i * rows : (i + 1) * rows, left : left + CB]
                layer(mix, self.rate, coef_ref, level)
            self.done = max(self.done, int(count))

    def step(i, ahead, state_ref, ascend=True, pending=None):
        cb = order(i)
        mu = cosf_ref[pl.ds(cb, 1), :]
        back = (0.5 * (0.5 * SSA_MAX)) * (1.0 - ASYM * mu)
        fall = wide(0.5 * SSA_MAX - back)
        back = wide(back)
        zero = jnp.zeros((gpoints, CB), jnp.float32)
        carry = (solar * mu, zero, zero)
        lit = litf_ref[pl.ds(cb, 1), :]
        if ascend:
            albedo = [albedo_ref[s, pl.ds(cb, 1), :] for s in range(2)]
        following = None
        if ahead:
            following = Prepare(rate_of(order(i + 1)))
            later = not isinstance(i, int) or i + 2 < ncb
            if later:
                for pair in range(2):
                    stage_pair(order(jnp.minimum(i + 2, ncb - 1)), pair)
                for pair in range(2):
                    product(inputs_ref.at[pair], big_ref, next_ref.at[pair])
        share = 0.78 if ascend else 1.0
        for level in range(lev):
            if pending is not None:
                pending.level(lev - 1 - level)
            carry = recur(coef_ref, level, state_ref, level, back, fall, carry)
            if following is not None:
                following.until(share * (level + 1))
        if not ascend:
            mix_ref[...] = next_ref[...]
            return carry
        up = Ascent(albedo, lit, carry, state_ref, rise_ref.at[0])
        for level in range(lev):
            up.level(lev - 1 - level)
            if following is not None:
                following.until(lev * (share + (1.0 - share) * (level + 1) / lev) + 1e-6)
        if following is not None and later:
            mix_ref[...] = next_ref[...]
        flux_ref[cb + 1] = rise_ref[0]

    pl.semaphore_wait(barrier, n - 1)
    sends = []
    for i, peer in enumerate(peers):
        copy = pltpu.make_async_remote_copy(
            src_ref=mine_ref,
            dst_ref=pieces_ref.at[i],
            send_sem=send_sem.at[i],
            recv_sem=recv_sem.at[i],
            device_id={"blk": peer},
            device_id_type=mesh_id,
        )
        copy.start()
        sends.append(copy)

    load.wait()
    multiply(0, mix_ref)
    Prepare(rate_of(0)).until(lev)
    multiply(order(1), mix_ref)
    carry = step(0, True, first_ref, ascend=False)
    for i in range(3):
        end_ref[i] = carry[i]

    for copy in sends:
        copy.wait()
    start_span = me * (ncb * CB // span)
    pieces = [mine_ref[...]] + [pieces_ref[i] for i in range(n - 1)]
    direct, diffuse = pick_albedo(pieces, start_span, span, blocks, ncb)
    albedo_ref[0] = direct
    albedo_ref[1] = diffuse
    pending = Ascent(
        [albedo_ref[s, 0:1, :] for s in range(2)], litf_ref[0:1, :], [end_ref[i] for i in range(3)],
        first_ref, rise_ref.at[1],
    )
    step(1, True, state_ref, pending=pending)
    flux_ref[1] = rise_ref[1]
    edge_ref[0] = rise_ref[1]
    edge_ref[1] = rise_ref[0]
    sends = []
    for i, peer in ((0, peers[-1]), (1, peers[0])):
        copy = pltpu.make_async_remote_copy(
            src_ref=edge_ref.at[i],
            dst_ref=halo_ref.at[i],
            send_sem=edge_send.at[i],
            recv_sem=edge_recv.at[i],
            device_id={"blk": peer},
            device_id_type=mesh_id,
        )
        copy.start()
        sends.append(copy)

    def middle_steps(i, unused):
        step(i, True, state_ref)
        return unused

    lax.fori_loop(2, ncb - 1, middle_steps, 0)
    step(ncb - 1, False, state_ref)
    for copy in sends:
        copy.wait()
    flux_ref[0] = halo_ref[1]
    flux_ref[ncb + 1] = halo_ref[0]


def side_kernel(flux_ref, neighbours_ref, weights_ref, out_ref):
    interfaces, parts, cols = out_ref.shape
    ncb = cols // CB
    rows = flux_ref.shape[1]
    start = (lax.axis_index("grp") * lax.axis_size("blk") + lax.axis_index("blk")) * cols
    for cb in range(ncb):
        own = slice(cb * CB, (cb + 1) * CB)
        picked = neighbours_ref[:, own] - (start + (cb - 1) * CB)
        weights = weights_ref[:, own]
        lanes, blocks, shares = [], [], []
        for k in range(3):
            row = jnp.broadcast_to(picked[k : k + 1], (8, CB))
            lanes.append(row & (CB - 1))
            blocks.append(row // CB)
            shares.append(jnp.broadcast_to(weights[k : k + 1], (8, CB)))
        results = [flux_ref[cb + 1, r : r + 8, :] for r in range(0, rows, 8)]
        for k in range(3):
            for i, r in enumerate(range(0, rows, 8)):
                near = [flux_ref[cb + j, r : r + 8, :] for j in range(3)]
                before, here, after = [
                    jnp.take_along_axis(v, lanes[k], axis=1, mode="promise_in_bounds") for v in near
                ]
                beside = jnp.where(blocks[k] == 0, before, jnp.where(blocks[k] == 1, here, after))
                results[i] = results[i] + shares[k] * (beside - near[1])
        for r, result in zip(range(0, rows, 8), results):
            top = r // parts
            count = min(8 // parts, interfaces - top)
            out_ref[top : top + count, :, own] = result[: count * parts].reshape(count, parts, CB)


def local(
    gas_state, cos_zenith, daylit, fine_area, fine_albedo, parent_of,
    optics_weight, solar_weight, neighbours, side_weight,
):
    n = lax.axis_size("blk")
    feats, lev, cols = gas_state.shape
    gpoints = solar_weight.shape[0]
    ncb = cols // CB
    blocks = fine_area.shape[0] // FB
    span = cols // blocks
    rows = round_up(2 * (lev + 1), 8)
    full = pl.BlockSpec(memory_space=VMEM)
    state = VMEM((4, lev, gpoints, CB), jnp.float32)
    fluxes = pl.pallas_call(
        functools.partial(flux_kernel, n, span),
        out_shape=jax.ShapeDtypeStruct((ncb + 2, rows, CB), jnp.float32),
        in_specs=[pl.BlockSpec(memory_space=pltpu.HBM)] + [full] * 7,
        out_specs=full,
        scratch_shapes=[
            VMEM((CHUNK * 2 * gpoints, 2 * CHUNK * feats), jnp.bfloat16),
            state,
            state,
            VMEM((3, gpoints, CB), jnp.float32),
            VMEM((2, ncb, CB), jnp.float32),
            VMEM((ncb, CB), jnp.float32),
            VMEM((ncb, CB), jnp.float32),
            VMEM((span + 8, 128), jnp.float32),
            VMEM((n - 1, span + 8, 128), jnp.float32),
            VMEM((2, rows, CB), jnp.float32),
            VMEM((2, rows, CB), jnp.float32),
            VMEM((2, CHUNK * feats, 2 * CB), gas_state.dtype),
            VMEM((2, CHUNK * 2 * gpoints, 2 * CB), jnp.float32),
            VMEM((2, CHUNK * 2 * gpoints, 2 * CB), jnp.float32),
            VMEM((6, lev, gpoints, CB), jnp.float32),
            VMEM((2, rows, CB), jnp.float32),
            VMEM((feats, lev, cols), gas_state.dtype),
            pltpu.SemaphoreType.DMA((n - 1,)),
            pltpu.SemaphoreType.DMA((n - 1,)),
            pltpu.SemaphoreType.DMA((2,)),
            pltpu.SemaphoreType.DMA((2,)),
            pltpu.SemaphoreType.DMA,
        ],
        compiler_params=pltpu.CompilerParams(
            collective_id=0, has_side_effects=True, vmem_limit_bytes=24 << 20
        ),
    )(*[
        pltpu.with_memory_space_constraint(value, pltpu.HBM)
        for value in (
            gas_state, cos_zenith.reshape(ncb, CB), daylit.reshape(ncb, CB), optics_weight.T,
            solar_weight.reshape(1, gpoints), fine_area.reshape(blocks, FB), fine_albedo,
            parent_of.reshape(blocks, FB),
        )
    ])
    result = pl.pallas_call(
        side_kernel,
        out_shape=jax.ShapeDtypeStruct((lev + 1, 2, cols), jnp.float32),
        in_specs=[full] * 3,
        out_specs=full,
        compiler_params=pltpu.CompilerParams(vmem_limit_bytes=8 << 20),
    )(fluxes, neighbours, side_weight)
    return jnp.transpose(result, (1, 0, 2))


def solution(mesh):
    columns = P(("grp", "blk"))
    last = P(None, ("grp", "blk"))
    in_specs = (
        P(None, None, ("grp", "blk")), columns, columns, columns, last, columns, P(), P(), last, last,
    )
    out_specs = P(None, None, ("grp", "blk"))
    return jax.shard_map(local, mesh=mesh, in_specs=in_specs, out_specs=out_specs, check_vma=False)
```

```python
import functools
import math

import jax
import jax.numpy as jnp
from jax import lax
from jax.experimental import pallas as pl
from jax.experimental.pallas import tpu as pltpu
from jax.sharding import PartitionSpec as P

CB = 128
FB = 128
ASYM = 0.8
TAU_SCALE = 0.08
SSA_MAX = 0.98
LOG2E = math.log2(math.e)
CHUNK = 8
VMEM = pltpu.VMEM
GROUND = 2.0 / SSA_MAX - 1.0
DEPTH = 0.5 * TAU_SCALE * math.log(2.0) * SSA_MAX


def round_up(value, multiple):
    return -(-value // multiple) * multiple


def local_albedo(area_ref, albedo_ref, parent_ref, span):
    blocks = area_ref.shape[0]
    area = area_ref[...]
    rows = [
        jnp.concatenate([albedo_ref[s : s + 1, b * FB : (b + 1) * FB] for b in range(blocks)], axis=0)
        for s in range(2)
    ]
    weights = jnp.transpose(jnp.concatenate([area, area * rows[0], area * rows[1]], axis=0))
    parent = jnp.transpose(jnp.concatenate([parent_ref[...]] * 3, axis=0))
    inside = parent & (span - 1)
    totals = jnp.concatenate(
        [jnp.sum(jnp.where(inside == j, weights, 0.0), axis=0, keepdims=True) for j in range(span)], axis=0
    )
    share = totals[:, :blocks]
    first = (totals[:, blocks : 2 * blocks] / share).astype(jnp.bfloat16).astype(jnp.float32)
    second = (totals[:, 2 * blocks :] / share).astype(jnp.bfloat16).astype(jnp.float32)
    number = (parent[0:1, :blocks] // span).astype(jnp.float32)
    return first, second, number


def pick_albedo(pieces, start_span, span, blocks, ncb):
    per = CB // span
    table = jnp.concatenate(
        [jnp.concatenate([p[0:span, s * blocks : (s + 1) * blocks] for p in pieces], axis=1) for s in range(2)],
        axis=0,
    ).astype(jnp.bfloat16)
    number = jnp.concatenate([p[span : span + 1, 0:blocks] for p in pieces], axis=1).astype(jnp.int32)
    total = number.shape[1]
    row = lax.broadcasted_iota(jnp.int32, (ncb, total), 0) * per + start_span
    parts = []
    for m in range(per):
        chosen = (number == row + m).astype(jnp.float32).astype(jnp.bfloat16)
        parts.append(
            lax.dot_general(chosen, table, (((1,), (1,)), ((), ())), preferred_element_type=jnp.float32)
        )
    direct = jnp.concatenate([p[:, 0:span] for p in parts], axis=1)
    diffuse = jnp.concatenate([p[:, span : 2 * span] for p in parts], axis=1)
    return direct, diffuse


def expand_weight(weight_ref, big_ref):
    feats, rows = weight_ref.shape
    wide = big_ref.shape[1]
    source = lax.broadcasted_iota(jnp.int32, (feats, wide), 0)
    column = lax.broadcasted_iota(jnp.int32, (feats, wide), 1)
    spread = (column % (wide // 2) // CHUNK == source).astype(jnp.float32).astype(jnp.bfloat16)
    repeated = lax.dot_general(
        weight_ref[...], spread, (((0,), (0,)), ((), ())), preferred_element_type=jnp.float32
    )
    row = lax.broadcasted_iota(jnp.int32, (rows, wide), 0)
    place = lax.broadcasted_iota(jnp.int32, (rows, wide), 1)
    scaled = jnp.where(row < rows // 2, LOG2E * repeated, 0.5 * repeated)
    high = scaled.astype(jnp.bfloat16).astype(jnp.float32)
    scaled = jnp.where(place < wide // 2, high, scaled - high)
    level = place % CHUNK
    for l in range(CHUNK):
        big_ref[l * rows : (l + 1) * rows, :] = jnp.where(level == l, scaled, 0.0).astype(jnp.bfloat16)


def stage(block, first, gas_ref, inputs_ref):
    feats = gas_ref.shape[0]
    cols = pl.ds(pl.multiple_of(block * CB, CB), CB)
    inputs_ref[...] = jnp.concatenate(
        [
            gas_ref[:, level : level + CHUNK, cols].reshape(feats * CHUNK, CB)
            for level in (first, first + CHUNK)
        ],
        axis=1,
    )


def product(inputs_ref, big_ref, mix_ref):
    inputs = inputs_ref[...]
    mix_ref[...] = jnp.dot(
        big_ref[...], jnp.concatenate([inputs, inputs], axis=0), preferred_element_type=jnp.float32
    )


def layer(mix, rate, back, fall, carry, state_ref, level):
    gpoints = mix.shape[0] // 2
    direct, big_b, big_q = carry
    x = mix[:gpoints]
    soft = jnp.maximum(x, lax.log2(1.0 + jnp.exp2(jnp.minimum(x, 100.0))))
    below = direct * jnp.exp2(soft * rate)
    u = jnp.tanh(mix[gpoints:])
    wide = 1.0 + u
    less = GROUND - u
    gap = (0.75 * (1.0 - ASYM)) * wide
    more = less + gap
    square = less * more
    inverse = lax.rsqrt(square)
    bend = jnp.tanh(((square * inverse) * soft) * DEPTH)
    slope = bend * inverse
    total = (less + more) * slope
    r = gap * slope
    bend2 = bend * bend
    plus = 1.0 + bend2
    scattered = wide * (direct - below)
    rising = scattered * back
    falling = scattered * fall
    state_ref[2, level] = big_b
    state_ref[3, level] = big_q + direct
    z = 1.0 / ((plus + total) - r * big_b)
    h = (big_q + big_b * rising) * z
    t2 = 1.0 - bend2
    state_ref[0, level] = t2 * z
    state_ref[1, level] = r * h + rising
    return below, (r + (plus - total) * big_b) * z, t2 * h + falling


def fold(parts):
    place = lax.broadcasted_iota(jnp.int32, parts[0].shape, 0)
    distance = 1
    while len(parts) > 1:
        even = (place & distance) == 0
        parts = [
            jnp.where(even, p, q) + pltpu.roll(jnp.where(even, q, p), 8 - distance, 0)
            for p, q in zip(parts[0::2], parts[1::2])
        ]
        distance *= 2
    rest = parts[0]
    while distance < 8:
        rest = rest + pltpu.roll(rest, 8 - distance, 0)
        distance *= 2
    return rest


def gather_g(value):
    parts = [value[i : i + 8] for i in range(0, value.shape[0], 8)]
    while len(parts) > 1:
        parts = [p + q for p, q in zip(parts[0::2], parts[1::2])]
    return parts[0]


class Ascent:
    def __init__(self, albedo, lit, carry, state_ref, rise_ref):
        lev = state_ref.shape[1]
        self.state_ref, self.rise_ref, self.lit = state_ref, rise_ref, lit
        direct, big_b, big_q = carry
        self.up = (albedo[1] * big_q + albedo[0] * direct) / (1.0 - albedo[1] * big_b)
        last = fold([gather_g(big_b * self.up + big_q + direct), gather_g(self.up)])
        rise_ref[2 * lev : 2 * lev + 8, :] = last * lit
        self.parts = []

    def level(self, level):
        state_ref = self.state_ref
        self.up = state_ref[0, level] * self.up + state_ref[1, level]
        down = state_ref[2, level] * self.up + state_ref[3, level]
        self.parts = [gather_g(down), gather_g(self.up)] + self.parts
        if level % 4 == 0:
            self.rise_ref[2 * level : 2 * level + 8, :] = fold(self.parts) * self.lit
            self.parts = []


def solar_column(solar_ref):
    row = solar_ref[...]
    n = row.shape[1]
    diagonal = lax.broadcasted_iota(jnp.int32, (n, n), 0) == lax.broadcasted_iota(jnp.int32, (n, n), 1)
    return jnp.sum(jnp.where(diagonal, row, 0.0), axis=1, keepdims=True)


def flux_kernel(
    n, span, gas_hbm, cos_ref, lit_ref, weight_ref, solar_ref, area_ref, fine_albedo_ref, parent_ref,
    flux_ref, big_ref, states_ref, end_ref, albedo_ref, cosf_ref, litf_ref, mine_ref, pieces_ref,
    edge_ref, halo_ref, inputs_ref, mix_ref, next_ref, gas_ref, send_sem, recv_sem, edge_send, edge_recv, gas_sem,
):
    ncb = cos_ref.shape[0]
    blocks = area_ref.shape[0]
    lev = gas_ref.shape[1]
    gpoints = solar_ref.shape[1]
    rows = 2 * gpoints
    slots = states_ref.shape[0]
    me = lax.axis_index("blk")
    peers = [lax.rem(me + shift, n) for shift in range(1, n)]
    mesh_id = pl.DeviceIdType.MESH

    load = pltpu.make_async_copy(gas_hbm, gas_ref, gas_sem)
    load.start()
    barrier = pltpu.get_barrier_semaphore()
    for peer in peers:
        pl.semaphore_signal(barrier, inc=1, device_id={"blk": peer}, device_id_type=mesh_id)

    first, second, number = local_albedo(area_ref, fine_albedo_ref, parent_ref, span)
    mine_ref[...] = jnp.zeros_like(mine_ref)
    mine_ref[0:span, 0:blocks] = first
    mine_ref[0:span, blocks : 2 * blocks] = second
    mine_ref[span : span + 1, 0:blocks] = number
    expand_weight(weight_ref, big_ref)
    cosf_ref[...] = cos_ref[...].astype(jnp.float32)
    litf_ref[...] = lit_ref[...].astype(jnp.float32)
    solar = solar_column(solar_ref)

    def order(i):
        if isinstance(i, int):
            return i * (ncb - 1) if i < 2 else i - 1
        return jnp.where(i < 2, i * (ncb - 1), i - 1)

    def wide(row):
        return jnp.broadcast_to(row, (gpoints, CB))

    def stage_pair(cb, pair):
        stage(cb, 2 * pair * CHUNK, gas_ref, inputs_ref.at[pair])

    def down(i, mix_ref, next_ref):
        cb = order(i)
        slot = lax.rem(i, slots)
        state_ref = states_ref.at[slot]
        mu = cosf_ref[pl.ds(cb, 1), :]
        rate = wide((-TAU_SCALE) / mu)
        back = (0.5 * (0.5 * SSA_MAX)) * (1.0 - ASYM * mu)
        fall = wide(0.5 * SSA_MAX - back)
        back = wide(back)
        zero = jnp.zeros((gpoints, CB), jnp.float32)
        carry = (solar * mu, zero, zero)
        after = order(jnp.minimum(i + 1, ncb - 1))
        for pair in range(2):
            stage_pair(after, pair)
        for pair in range(2):
            product(inputs_ref.at[pair], big_ref, next_ref.at[pair])
        for level in range(lev):
            chunk, j = level // CHUNK, level % CHUNK
            left = chunk % 2 * CB
            mix = mix_ref[chunk // 2, j * rows : (j + 1) * rows, left : left + CB]
            carry = layer(mix, rate, back, fall, carry, state_ref, level)
        for j in range(3):
            end_ref[slot, j] = carry[j]

    def up(i):
        cb = order(i)
        slot = lax.rem(i, slots)
        albedo = [albedo_ref[s, pl.ds(cb, 1), :] for s in range(2)]
        rise = Ascent(
            albedo, litf_ref[pl.ds(cb, 1), :], [end_ref[slot, j] for j in range(3)],
            states_ref.at[slot], flux_ref.at[cb + 1],
        )
        for level in reversed(range(lev)):
            rise.level(level)

    load.wait()
    for pair in range(2):
        stage_pair(0, pair)
        product(inputs_ref.at[pair], big_ref, mix_ref.at[pair])
    pl.semaphore_wait(barrier, n - 1)
    sends = []
    for i, peer in enumerate(peers):
        copy = pltpu.make_async_remote_copy(
            src_ref=mine_ref,
            dst_ref=pieces_ref.at[i],
            send_sem=send_sem.at[i],
            recv_sem=recv_sem.at[i],
            device_id={"blk": peer},
            device_id_type=mesh_id,
        )
        copy.start()
        sends.append(copy)

    edges = [
        pltpu.make_async_remote_copy(
            src_ref=edge_ref.at[i],
            dst_ref=halo_ref.at[i],
            send_sem=edge_send.at[i],
            recv_sem=edge_recv.at[i],
            device_id={"blk": peer},
            device_id_type=mesh_id,
        )
        for i, peer in ((0, peers[-1]), (1, peers[0]))
    ]

    def early_up(i, unused):
        up(i)

        @pl.when(i == 1)
        def _():
            edge_ref[0] = flux_ref[1]
            edge_ref[1] = flux_ref[ncb]
            for copy in edges:
                copy.start()

        return unused

    def receive():
        for copy in sends:
            copy.wait()
        start_span = me * (ncb * CB // span)
        pieces = [mine_ref[...]] + [pieces_ref[i] for i in range(n - 1)]
        direct, diffuse = pick_albedo(pieces, start_span, span, blocks, ncb)
        albedo_ref[0] = direct
        albedo_ref[1] = diffuse
        lax.fori_loop(0, slots, early_up, 0)

    def two_steps(j, unused):
        down(2 * j, mix_ref, next_ref)

        @pl.when(j == 1)
        def _():
            receive()

        @pl.when(j > 1)
        def _():
            up(2 * j)

        down(2 * j + 1, next_ref, mix_ref)

        @pl.when(j > 0)
        def _():
            up(2 * j + 1)

        return unused

    lax.fori_loop(0, ncb // 2, two_steps, 0)
    for copy in edges:
        copy.wait()
    flux_ref[0] = halo_ref[1]
    flux_ref[ncb + 1] = halo_ref[0]


def side_kernel(flux_ref, neighbours_ref, weights_ref, out_ref):
    interfaces, parts, cols = out_ref.shape
    ncb = cols // CB
    rows = flux_ref.shape[1]
    start = (lax.axis_index("grp") * lax.axis_size("blk") + lax.axis_index("blk")) * cols
    for cb in range(ncb):
        own = slice(cb * CB, (cb + 1) * CB)
        picked = neighbours_ref[:, own] - (start + (cb - 1) * CB)
        weights = weights_ref[:, own]
        lanes, blocks, shares = [], [], []
        for k in range(3):
            row = jnp.broadcast_to(picked[k : k + 1], (8, CB))
            lanes.append(row & (CB - 1))
            blocks.append(row // CB)
            shares.append(jnp.broadcast_to(weights[k : k + 1], (8, CB)))
        results = [flux_ref[cb + 1, r : r + 8, :] for r in range(0, rows, 8)]
        for k in range(3):
            for i, r in enumerate(range(0, rows, 8)):
                near = [flux_ref[cb + j, r : r + 8, :] for j in range(3)]
                before, here, after = [
                    jnp.take_along_axis(v, lanes[k], axis=1, mode="promise_in_bounds") for v in near
                ]
                beside = jnp.where(blocks[k] == 0, before, jnp.where(blocks[k] == 1, here, after))
                results[i] = results[i] + shares[k] * (beside - near[1])
        for r, result in zip(range(0, rows, 8), results):
            top = r // parts
            count = min(8 // parts, interfaces - top)
            out_ref[top : top + count, :, own] = result[: count * parts].reshape(count, parts, CB)


def local(
    gas_state, cos_zenith, daylit, fine_area, fine_albedo, parent_of,
    optics_weight, solar_weight, neighbours, side_weight,
):
    n = lax.axis_size("blk")
    feats, lev, cols = gas_state.shape
    gpoints = solar_weight.shape[0]
    ncb = cols // CB
    blocks = fine_area.shape[0] // FB
    span = cols // blocks
    rows = round_up(2 * (lev + 1), 8)
    full = pl.BlockSpec(memory_space=VMEM)
    slots = 3
    fluxes = pl.pallas_call(
        functools.partial(flux_kernel, n, span),
        out_shape=jax.ShapeDtypeStruct((ncb + 2, rows, CB), jnp.float32),
        in_specs=[pl.BlockSpec(memory_space=pltpu.HBM)] + [full] * 7,
        out_specs=full,
        scratch_shapes=[
            VMEM((CHUNK * 2 * gpoints, 2 * CHUNK * feats), jnp.bfloat16),
            VMEM((slots, 4, lev, gpoints, CB), jnp.float32),
            VMEM((slots, 3, gpoints, CB), jnp.float32),
            VMEM((2, ncb, CB), jnp.float32),
            VMEM((ncb, CB), jnp.float32),
            VMEM((ncb, CB), jnp.float32),
            VMEM((span + 8, 128), jnp.float32),
            VMEM((n - 1, span + 8, 128), jnp.float32),
            VMEM((2, rows, CB), jnp.float32),
            VMEM((2, rows, CB), jnp.float32),
            VMEM((2, CHUNK * feats, 2 * CB), gas_state.dtype),
            VMEM((2, CHUNK * 2 * gpoints, 2 * CB), jnp.float32),
            VMEM((2, CHUNK * 2 * gpoints, 2 * CB), jnp.float32),
            VMEM((feats, lev, cols), gas_state.dtype),
            pltpu.SemaphoreType.DMA((n - 1,)),
            pltpu.SemaphoreType.DMA((n - 1,)),
            pltpu.SemaphoreType.DMA((2,)),
            pltpu.SemaphoreType.DMA((2,)),
            pltpu.SemaphoreType.DMA,
        ],
        compiler_params=pltpu.CompilerParams(
            collective_id=0, has_side_effects=True, vmem_limit_bytes=24 << 20
        ),
    )(*[
        pltpu.with_memory_space_constraint(value, pltpu.HBM)
        for value in (
            gas_state, cos_zenith.reshape(ncb, CB), daylit.reshape(ncb, CB), optics_weight.T,
            solar_weight.reshape(1, gpoints), fine_area.reshape(blocks, FB), fine_albedo,
            parent_of.reshape(blocks, FB),
        )
    ])
    result = pl.pallas_call(
        side_kernel,
        out_shape=jax.ShapeDtypeStruct((lev + 1, 2, cols), jnp.float32),
        in_specs=[full] * 3,
        out_specs=full,
        compiler_params=pltpu.CompilerParams(vmem_limit_bytes=8 << 20),
    )(fluxes, neighbours, side_weight)
    return jnp.transpose(result, (1, 0, 2))


def solution(mesh):
    columns = P(("grp", "blk"))
    last = P(None, ("grp", "blk"))
    in_specs = (
        P(None, None, ("grp", "blk")), columns, columns, columns, last, columns, P(), P(), last, last,
    )
    out_specs = P(None, None, ("grp", "blk"))
    return jax.shard_map(local, mesh=mesh, in_specs=in_specs, out_specs=out_specs, check_vma=False)
```

```python
import functools
import math

import jax
import jax.numpy as jnp
from jax import lax
from jax.experimental import pallas as pl
from jax.experimental.pallas import tpu as pltpu
from jax.sharding import PartitionSpec as P

CB = 128
FB = 128
ASYM = 0.8
TAU_SCALE = 0.08
SSA_MAX = 0.98
LOG2E = math.log2(math.e)
CHUNK = 8
VMEM = pltpu.VMEM
GROUND = 2.0 / SSA_MAX - 1.0
DEPTH = 0.5 * TAU_SCALE * math.log(2.0) * SSA_MAX


def round_up(value, multiple):
    return -(-value // multiple) * multiple


def local_albedo(area_ref, albedo_ref, parent_ref, span):
    blocks = area_ref.shape[0]
    area = area_ref[...]
    rows = [
        jnp.concatenate([albedo_ref[s : s + 1, b * FB : (b + 1) * FB] for b in range(blocks)], axis=0)
        for s in range(2)
    ]
    weights = jnp.transpose(jnp.concatenate([area, area * rows[0], area * rows[1]], axis=0))
    parent = jnp.transpose(jnp.concatenate([parent_ref[...]] * 3, axis=0))
    inside = parent & (span - 1)
    totals = jnp.concatenate(
        [jnp.sum(jnp.where(inside == j, weights, 0.0), axis=0, keepdims=True) for j in range(span)], axis=0
    )
    share = totals[:, :blocks]
    first = (totals[:, blocks : 2 * blocks] / share).astype(jnp.bfloat16).astype(jnp.float32)
    second = (totals[:, 2 * blocks :] / share).astype(jnp.bfloat16).astype(jnp.float32)
    number = (parent[0:1, :blocks] // span).astype(jnp.float32)
    return first, second, number


def own_piece(first, second, number, mine_ref):
    span = first.shape[0]
    per = CB // span
    blocks = first.shape[1]
    for i, values in enumerate((first, second)):
        tiled = jnp.transpose(jnp.concatenate([values] * per, axis=0))
        mine_ref[i * blocks : (i + 1) * blocks, :] = tiled.astype(jnp.bfloat16)
    tail = mine_ref.shape[0] - 2 * blocks
    numbers = jnp.concatenate([number] * (CB // blocks), axis=1)
    mine_ref[2 * blocks :, :] = jnp.broadcast_to(numbers, (tail, CB)).astype(jnp.bfloat16)


def pick_albedo(pieces, start_span, span, blocks, ncb):
    per = CB // span
    group = CB // blocks
    lane = lax.broadcasted_iota(jnp.int32, (per * ncb, CB), 1)
    row = lax.broadcasted_iota(jnp.int32, (per * ncb, CB), 0)
    wanted = (row % ncb * per + row // ncb + start_span).astype(jnp.float32)
    total = None
    for first in range(0, len(pieces), group):
        members = pieces[first : first + group]
        number = jnp.full((per * ncb, CB), -1.0, jnp.float32)
        for q, piece in enumerate(members):
            row_of = piece[2 * blocks :, :].astype(jnp.float32)[0:1]
            number = jnp.where(lane // blocks == q, row_of, number)
        chosen = (number == wanted).astype(jnp.float32).astype(jnp.bfloat16)
        chosen = chosen[:, : len(members) * blocks]
        table = jnp.concatenate(
            [
                jnp.concatenate([piece[i * blocks : (i + 1) * blocks, :] for piece in members], axis=0)
                for i in range(2)
            ],
            axis=1,
        )
        part = jnp.dot(chosen, table, preferred_element_type=jnp.float32)
        total = part if total is None else total + part
    lane = lax.broadcasted_iota(jnp.int32, (ncb, CB), 1)
    results = []
    for i in range(2):
        result = total[0:ncb, i * CB : (i + 1) * CB]
        for m in range(1, per):
            part = total[m * ncb : (m + 1) * ncb, i * CB : (i + 1) * CB]
            result = jnp.where(lane // span == m, part, result)
        results.append(result)
    return results


def expand_weight(weight_ref, big_ref):
    feats, rows = weight_ref.shape
    wide = big_ref.shape[1]
    source = lax.broadcasted_iota(jnp.int32, (feats, wide), 0)
    column = lax.broadcasted_iota(jnp.int32, (feats, wide), 1)
    spread = (column % (wide // 2) // CHUNK == source).astype(jnp.float32).astype(jnp.bfloat16)
    repeated = lax.dot_general(
        weight_ref[...], spread, (((0,), (0,)), ((), ())), preferred_element_type=jnp.float32
    )
    row = lax.broadcasted_iota(jnp.int32, (rows, wide), 0)
    place = lax.broadcasted_iota(jnp.int32, (rows, wide), 1)
    scaled = jnp.where(row < rows // 2, LOG2E * repeated, 0.5 * repeated)
    high = scaled.astype(jnp.bfloat16).astype(jnp.float32)
    scaled = jnp.where(place < wide // 2, high, scaled - high)
    level = place % CHUNK
    for l in range(CHUNK):
        big_ref[l * rows : (l + 1) * rows, :] = jnp.where(level == l, scaled, 0.0).astype(jnp.bfloat16)


def stage(block, first, gas_ref, inputs_ref):
    feats = gas_ref.shape[0]
    cols = pl.ds(pl.multiple_of(block * CB, CB), CB)
    inputs_ref[...] = jnp.concatenate(
        [
            gas_ref[:, level : level + CHUNK, cols].reshape(feats * CHUNK, CB)
            for level in (first, first + CHUNK)
        ],
        axis=1,
    )


def product(inputs_ref, big_ref, mix_ref):
    inputs = inputs_ref[...]
    mix_ref[...] = jnp.dot(
        big_ref[...], jnp.concatenate([inputs, inputs], axis=0), preferred_element_type=jnp.float32
    )


def layer(mix, rate, back, fall, carry, state_ref, level):
    gpoints = mix.shape[0] // 2
    direct, big_b, big_q = carry
    x = mix[:gpoints]
    soft = jnp.maximum(x, lax.log2(1.0 + jnp.exp2(jnp.minimum(x, 100.0))))
    below = direct * jnp.exp2(soft * rate)
    u = jnp.tanh(mix[gpoints:])
    wide = 1.0 + u
    less = GROUND - u
    gap = (0.75 * (1.0 - ASYM)) * wide
    more = less + gap
    square = less * more
    inverse = lax.rsqrt(square)
    bend = jnp.tanh(((square * inverse) * soft) * DEPTH)
    slope = bend * inverse
    total = (less + more) * slope
    r = gap * slope
    bend2 = bend * bend
    plus = 1.0 + bend2
    scattered = wide * (direct - below)
    rising = scattered * back
    falling = scattered * fall
    state_ref[2, level] = big_b
    state_ref[3, level] = big_q + direct
    z = 1.0 / ((plus + total) - r * big_b)
    h = (big_q + big_b * rising) * z
    t2 = 1.0 - bend2
    state_ref[0, level] = t2 * z
    state_ref[1, level] = r * h + rising
    return below, (r + (plus - total) * big_b) * z, t2 * h + falling


def fold(parts):
    place = lax.broadcasted_iota(jnp.int32, parts[0].shape, 0)
    distance = 1
    while len(parts) > 1:
        even = (place & distance) == 0
        parts = [
            jnp.where(even, p, q) + pltpu.roll(jnp.where(even, q, p), 8 - distance, 0)
            for p, q in zip(parts[0::2], parts[1::2])
        ]
        distance *= 2
    rest = parts[0]
    while distance < 8:
        rest = rest + pltpu.roll(rest, 8 - distance, 0)
        distance *= 2
    return rest


def gather_g(value):
    parts = [value[i : i + 8] for i in range(0, value.shape[0], 8)]
    while len(parts) > 1:
        parts = [p + q for p, q in zip(parts[0::2], parts[1::2])]
    return parts[0]


class Ascent:
    def __init__(self, albedo, lit, carry, state_ref, rise_ref):
        lev = state_ref.shape[1]
        self.state_ref, self.rise_ref, self.lit = state_ref, rise_ref, lit
        direct, big_b, big_q = carry
        self.up = (albedo[1] * big_q + albedo[0] * direct) / (1.0 - albedo[1] * big_b)
        last = fold([gather_g(big_b * self.up + big_q + direct), gather_g(self.up)])
        rise_ref[2 * lev : 2 * lev + 8, :] = last * lit
        self.parts = []

    def level(self, level):
        state_ref = self.state_ref
        self.up = state_ref[0, level] * self.up + state_ref[1, level]
        down = state_ref[2, level] * self.up + state_ref[3, level]
        self.parts = [gather_g(down), gather_g(self.up)] + self.parts
        if level % 4 == 0:
            self.rise_ref[2 * level : 2 * level + 8, :] = fold(self.parts) * self.lit
            self.parts = []


def solar_column(solar_ref):
    row = solar_ref[...]
    n = row.shape[1]
    diagonal = lax.broadcasted_iota(jnp.int32, (n, n), 0) == lax.broadcasted_iota(jnp.int32, (n, n), 1)
    return jnp.sum(jnp.where(diagonal, row, 0.0), axis=1, keepdims=True)


def flux_kernel(
    n, span, gas_hbm, cos_hbm, lit_hbm, weight_hbm, solar_hbm, area_hbm, fine_albedo_hbm, parent_hbm,
    flux_ref, big_ref, states_ref, end_ref, albedo_ref, cosf_ref, litf_ref, mine_ref, pieces_ref,
    edge_ref, halo_ref, inputs_ref, mix_ref, next_ref, gas_ref, cos_ref, lit_ref, weight_ref, solar_ref,
    area_ref, fine_albedo_ref, parent_ref, send_sem, recv_sem, edge_send, edge_recv, load_sem,
):
    ncb = cos_ref.shape[0]
    blocks = area_ref.shape[0]
    lev = gas_ref.shape[1]
    gpoints = solar_ref.shape[1]
    rows = 2 * gpoints
    slots = states_ref.shape[0]
    me = lax.axis_index("blk")
    peers = [lax.rem(me + shift, n) for shift in range(1, n)]
    mesh_id = pl.DeviceIdType.MESH

    sources = [
        (weight_hbm, weight_ref), (parent_hbm, parent_ref), (area_hbm, area_ref),
        (fine_albedo_hbm, fine_albedo_ref), (solar_hbm, solar_ref), (cos_hbm, cos_ref), (lit_hbm, lit_ref),
        (gas_hbm.at[:, :, 0:CB], gas_ref.at[:, :, 0:CB]), (gas_hbm.at[:, :, CB:], gas_ref.at[:, :, CB:]),
    ]
    loads = [pltpu.make_async_copy(src, dst, load_sem.at[i]) for i, (src, dst) in enumerate(sources)]
    for load in loads:
        load.start()
    barrier = pltpu.get_barrier_semaphore()
    for peer in peers:
        pl.semaphore_signal(barrier, inc=1, device_id={"blk": peer}, device_id_type=mesh_id)

    for load in loads[:-1]:
        load.wait()
    expand_weight(weight_ref, big_ref)
    for pair in range(2):
        stage(0, 2 * pair * CHUNK, gas_ref, inputs_ref.at[pair])
        product(inputs_ref.at[pair], big_ref, mix_ref.at[pair])
    first, second, number = local_albedo(area_ref, fine_albedo_ref, parent_ref, span)
    own_piece(first, second, number, mine_ref)
    cosf_ref[...] = cos_ref[...].astype(jnp.float32)
    litf_ref[...] = lit_ref[...].astype(jnp.float32)
    solar = solar_column(solar_ref)
    loads[-1].wait()

    def order(i):
        if isinstance(i, int):
            return i * (ncb - 1) if i < 2 else i - 1
        return jnp.where(i < 2, i * (ncb - 1), i - 1)

    def wide(row):
        return jnp.broadcast_to(row, (gpoints, CB))

    def stage_pair(cb, pair):
        stage(cb, 2 * pair * CHUNK, gas_ref, inputs_ref.at[pair])

    def down(i, mix_ref, next_ref):
        cb = order(i)
        slot = lax.rem(i, slots)
        state_ref = states_ref.at[slot]
        mu = cosf_ref[pl.ds(cb, 1), :]
        rate = wide((-TAU_SCALE) / mu)
        back = (0.5 * (0.5 * SSA_MAX)) * (1.0 - ASYM * mu)
        fall = wide(0.5 * SSA_MAX - back)
        back = wide(back)
        zero = jnp.zeros((gpoints, CB), jnp.float32)
        carry = (solar * mu, zero, zero)
        after = order(jnp.minimum(i + 1, ncb - 1))
        for pair in range(2):
            stage_pair(after, pair)
        for pair in range(2):
            product(inputs_ref.at[pair], big_ref, next_ref.at[pair])
        for level in range(lev):
            chunk, j = level // CHUNK, level % CHUNK
            left = chunk % 2 * CB
            mix = mix_ref[chunk // 2, j * rows : (j + 1) * rows, left : left + CB]
            carry = layer(mix, rate, back, fall, carry, state_ref, level)
        for j in range(3):
            end_ref[slot, j] = carry[j]

    def up(i):
        cb = order(i)
        slot = lax.rem(i, slots)
        albedo = [albedo_ref[s, pl.ds(cb, 1), :] for s in range(2)]
        rise = Ascent(
            albedo, litf_ref[pl.ds(cb, 1), :], [end_ref[slot, j] for j in range(3)],
            states_ref.at[slot], flux_ref.at[cb + 1],
        )
        for level in reversed(range(lev)):
            rise.level(level)

    sends = [
        pltpu.make_async_remote_copy(
            src_ref=mine_ref,
            dst_ref=pieces_ref.at[i],
            send_sem=send_sem.at[i],
            recv_sem=recv_sem.at[i],
            device_id={"blk": peer},
            device_id_type=mesh_id,
        )
        for i, peer in enumerate(peers)
    ]

    def send():
        pl.semaphore_wait(barrier, n - 1)
        for copy in sends:
            copy.start()

    lower = me < n // 2

    @pl.when(jnp.logical_not(lower))
    def _():
        send()

    edges = [
        pltpu.make_async_remote_copy(
            src_ref=edge_ref.at[i],
            dst_ref=halo_ref.at[i],
            send_sem=edge_send.at[i],
            recv_sem=edge_recv.at[i],
            device_id={"blk": peer},
            device_id_type=mesh_id,
        )
        for i, peer in ((0, peers[-1]), (1, peers[0]))
    ]

    def early_up(i, unused):
        up(i)

        @pl.when(i == 1)
        def _():
            edge_ref[0] = flux_ref[1]
            edge_ref[1] = flux_ref[ncb]
            for copy in edges:
                copy.start()

        return unused

    def receive():
        for copy in sends:
            copy.wait()
        start_span = me * (ncb * CB // span)
        pieces = [mine_ref] + [pieces_ref.at[i] for i in range(n - 1)]
        direct, diffuse = pick_albedo(pieces, start_span, span, blocks, ncb)
        albedo_ref[0] = direct
        albedo_ref[1] = diffuse
        lax.fori_loop(0, slots, early_up, 0)

    def two_steps(j, unused):
        down(2 * j, mix_ref, next_ref)

        @pl.when(j > 1)
        def _():
            up(2 * j)

        down(2 * j + 1, next_ref, mix_ref)

        @pl.when(jnp.logical_and(j == 0, lower))
        def _():
            send()

        @pl.when(j == 1)
        def _():
            receive()

        @pl.when(j > 1)
        def _():
            up(2 * j + 1)

        return unused

    lax.fori_loop(0, ncb // 2, two_steps, 0)
    for copy in edges:
        copy.wait()
    flux_ref[0] = halo_ref[1]
    flux_ref[ncb + 1] = halo_ref[0]


def side_kernel(flux_ref, neighbours_ref, weights_ref, out_ref):
    interfaces, parts, cols = out_ref.shape
    ncb = cols // CB
    rows = flux_ref.shape[1]
    start = (lax.axis_index("grp") * lax.axis_size("blk") + lax.axis_index("blk")) * cols
    for cb in range(ncb):
        own = slice(cb * CB, (cb + 1) * CB)
        picked = neighbours_ref[:, own] - (start + (cb - 1) * CB)
        weights = weights_ref[:, own]
        lanes, blocks, shares = [], [], []
        for k in range(3):
            row = jnp.broadcast_to(picked[k : k + 1], (8, CB))
            lanes.append(row & (CB - 1))
            blocks.append(row // CB)
            shares.append(jnp.broadcast_to(weights[k : k + 1], (8, CB)))
        results = [flux_ref[cb + 1, r : r + 8, :] for r in range(0, rows, 8)]
        for k in range(3):
            for i, r in enumerate(range(0, rows, 8)):
                near = [flux_ref[cb + j, r : r + 8, :] for j in range(3)]
                before, here, after = [
                    jnp.take_along_axis(v, lanes[k], axis=1, mode="promise_in_bounds") for v in near
                ]
                beside = jnp.where(blocks[k] == 0, before, jnp.where(blocks[k] == 1, here, after))
                results[i] = results[i] + shares[k] * (beside - near[1])
        for r, result in zip(range(0, rows, 8), results):
            top = r // parts
            count = min(8 // parts, interfaces - top)
            out_ref[top : top + count, :, own] = result[: count * parts].reshape(count, parts, CB)


def local(
    gas_state, cos_zenith, daylit, fine_area, fine_albedo, parent_of,
    optics_weight, solar_weight, neighbours, side_weight,
):
    n = lax.axis_size("blk")
    feats, lev, cols = gas_state.shape
    gpoints = solar_weight.shape[0]
    ncb = cols // CB
    blocks = fine_area.shape[0] // FB
    span = cols // blocks
    rows = round_up(2 * (lev + 1), 8)
    full = pl.BlockSpec(memory_space=VMEM)
    slots = 4
    fluxes = pl.pallas_call(
        functools.partial(flux_kernel, n, span),
        out_shape=jax.ShapeDtypeStruct((ncb + 2, rows, CB), jnp.float32),
        in_specs=[pl.BlockSpec(memory_space=pltpu.HBM)] * 8,
        out_specs=full,
        scratch_shapes=[
            VMEM((CHUNK * 2 * gpoints, 2 * CHUNK * feats), jnp.bfloat16),
            VMEM((slots, 4, lev, gpoints, CB), jnp.float32),
            VMEM((slots, 3, gpoints, CB), jnp.float32),
            VMEM((2, ncb, CB), jnp.float32),
            VMEM((ncb, CB), jnp.float32),
            VMEM((ncb, CB), jnp.float32),
            VMEM((2 * blocks + 16, CB), jnp.bfloat16),
            VMEM((n - 1, 2 * blocks + 16, CB), jnp.bfloat16),
            VMEM((2, rows, CB), jnp.float32),
            VMEM((2, rows, CB), jnp.float32),
            VMEM((2, CHUNK * feats, 2 * CB), gas_state.dtype),
            VMEM((2, CHUNK * 2 * gpoints, 2 * CB), jnp.float32),
            VMEM((2, CHUNK * 2 * gpoints, 2 * CB), jnp.float32),
            VMEM((feats, lev, cols), gas_state.dtype),
            VMEM((ncb, CB), cos_zenith.dtype),
            VMEM((ncb, CB), daylit.dtype),
            VMEM((feats, 2 * gpoints), optics_weight.dtype),
            VMEM((1, gpoints), jnp.float32),
            VMEM((blocks, FB), jnp.float32),
            VMEM(fine_albedo.shape, jnp.float32),
            VMEM((blocks, FB), parent_of.dtype),
            pltpu.SemaphoreType.DMA((n - 1,)),
            pltpu.SemaphoreType.DMA((n - 1,)),
            pltpu.SemaphoreType.DMA((2,)),
            pltpu.SemaphoreType.DMA((2,)),
            pltpu.SemaphoreType.DMA((9,)),
        ],
        compiler_params=pltpu.CompilerParams(
            collective_id=0, has_side_effects=True, vmem_limit_bytes=24 << 20
        ),
    )(*[
        pltpu.with_memory_space_constraint(value, pltpu.HBM)
        for value in (
            gas_state, cos_zenith.reshape(ncb, CB), daylit.reshape(ncb, CB), optics_weight.T,
            solar_weight.reshape(1, gpoints), fine_area.reshape(blocks, FB), fine_albedo,
            parent_of.reshape(blocks, FB),
        )
    ])
    result = pl.pallas_call(
        side_kernel,
        out_shape=jax.ShapeDtypeStruct((lev + 1, 2, cols), jnp.float32),
        in_specs=[full] * 3,
        out_specs=full,
        compiler_params=pltpu.CompilerParams(vmem_limit_bytes=8 << 20),
    )(fluxes, neighbours, side_weight)
    return jnp.transpose(result, (1, 0, 2))


def solution(mesh):
    columns = P(("grp", "blk"))
    last = P(None, ("grp", "blk"))
    in_specs = (
        P(None, None, ("grp", "blk")), columns, columns, columns, last, columns, P(), P(), last, last,
    )
    out_specs = P(None, None, ("grp", "blk"))
    return jax.shard_map(local, mesh=mesh, in_specs=in_specs, out_specs=out_specs, check_vma=False)
```

```python
import functools
import math

import jax
import jax.numpy as jnp
from jax import lax
from jax.experimental import pallas as pl
from jax.experimental.pallas import tpu as pltpu
from jax.sharding import PartitionSpec as P

CB = 128
FB = 128
ASYM = 0.8
TAU_SCALE = 0.08
SSA_MAX = 0.98
LOG2E = math.log2(math.e)
CHUNK = 8
VMEM = pltpu.VMEM
GROUND = 2.0 / SSA_MAX - 1.0
DEPTH = 0.5 * TAU_SCALE * math.log(2.0) * SSA_MAX


def round_up(value, multiple):
    return -(-value // multiple) * multiple


def local_albedo(area_ref, albedo_ref, parent_ref, span):
    blocks = area_ref.shape[0]
    area = area_ref[...]
    rows = [
        jnp.concatenate([albedo_ref[s : s + 1, b * FB : (b + 1) * FB] for b in range(blocks)], axis=0)
        for s in range(2)
    ]
    weights = jnp.transpose(jnp.concatenate([area, area * rows[0], area * rows[1]], axis=0))
    parent = jnp.transpose(jnp.concatenate([parent_ref[...]] * 3, axis=0))
    inside = parent & (span - 1)
    totals = jnp.concatenate(
        [jnp.sum(jnp.where(inside == j, weights, 0.0), axis=0, keepdims=True) for j in range(span)], axis=0
    )
    share = totals[:, :blocks]
    first = (totals[:, blocks : 2 * blocks] / share).astype(jnp.bfloat16).astype(jnp.float32)
    second = (totals[:, 2 * blocks :] / share).astype(jnp.bfloat16).astype(jnp.float32)
    number = (parent[0:1, :blocks] // span).astype(jnp.float32)
    return first, second, number


def own_piece(first, second, number, mine_ref):
    span = first.shape[0]
    per = CB // span
    blocks = first.shape[1]
    for i, values in enumerate((first, second)):
        tiled = jnp.transpose(jnp.concatenate([values] * per, axis=0))
        mine_ref[i * blocks : (i + 1) * blocks, :] = tiled.astype(jnp.bfloat16)
    tail = mine_ref.shape[0] - 2 * blocks
    numbers = jnp.concatenate([number] * (CB // blocks), axis=1)
    mine_ref[2 * blocks :, :] = jnp.broadcast_to(numbers, (tail, CB)).astype(jnp.bfloat16)


def pick_albedo(pieces, start_span, span, blocks, ncb):
    per = CB // span
    group = CB // blocks
    lane = lax.broadcasted_iota(jnp.int32, (per * ncb, CB), 1)
    row = lax.broadcasted_iota(jnp.int32, (per * ncb, CB), 0)
    wanted = (row % ncb * per + row // ncb + start_span).astype(jnp.float32)
    total = None
    for first in range(0, len(pieces), group):
        members = pieces[first : first + group]
        number = jnp.full((per * ncb, CB), -1.0, jnp.float32)
        for q, piece in enumerate(members):
            row_of = piece[2 * blocks :, :].astype(jnp.float32)[0:1]
            number = jnp.where(lane // blocks == q, row_of, number)
        chosen = (number == wanted).astype(jnp.float32).astype(jnp.bfloat16)
        chosen = chosen[:, : len(members) * blocks]
        table = jnp.concatenate(
            [
                jnp.concatenate([piece[i * blocks : (i + 1) * blocks, :] for piece in members], axis=0)
                for i in range(2)
            ],
            axis=1,
        )
        part = jnp.dot(chosen, table, preferred_element_type=jnp.float32)
        total = part if total is None else total + part
    lane = lax.broadcasted_iota(jnp.int32, (ncb, CB), 1)
    results = []
    for i in range(2):
        result = total[0:ncb, i * CB : (i + 1) * CB]
        for m in range(1, per):
            part = total[m * ncb : (m + 1) * ncb, i * CB : (i + 1) * CB]
            result = jnp.where(lane // span == m, part, result)
        results.append(result)
    return results


def expand_weight(weight_ref, big_ref):
    feats, rows = weight_ref.shape
    wide = big_ref.shape[1]
    source = lax.broadcasted_iota(jnp.int32, (feats, wide), 0)
    column = lax.broadcasted_iota(jnp.int32, (feats, wide), 1)
    spread = (column % (wide // 2) // CHUNK == source).astype(jnp.float32).astype(jnp.bfloat16)
    repeated = lax.dot_general(
        weight_ref[...], spread, (((0,), (0,)), ((), ())), preferred_element_type=jnp.float32
    )
    row = lax.broadcasted_iota(jnp.int32, (rows, wide), 0)
    place = lax.broadcasted_iota(jnp.int32, (rows, wide), 1)
    scaled = jnp.where(row < rows // 2, LOG2E * repeated, 0.5 * repeated)
    high = scaled.astype(jnp.bfloat16).astype(jnp.float32)
    scaled = jnp.where(place < wide // 2, high, scaled - high)
    level = place % CHUNK
    for l in range(CHUNK):
        big_ref[l * rows : (l + 1) * rows, :] = jnp.where(level == l, scaled, 0.0).astype(jnp.bfloat16)


def stage(block, first, gas_ref, inputs_ref):
    feats = gas_ref.shape[0]
    cols = pl.ds(pl.multiple_of(block * CB, CB), CB)
    inputs_ref[...] = jnp.concatenate(
        [
            gas_ref[:, level : level + CHUNK, cols].reshape(feats * CHUNK, CB)
            for level in (first, first + CHUNK)
        ],
        axis=1,
    )


def product(inputs_ref, big_ref, mix_ref):
    inputs = inputs_ref[...]
    mix_ref[...] = jnp.dot(
        big_ref[...], jnp.concatenate([inputs, inputs], axis=0), preferred_element_type=jnp.float32
    )


def layer(mix, rate, back, fall, carry, state_ref, level):
    gpoints = mix.shape[0] // 2
    direct, big_b, big_q = carry
    x = mix[:gpoints]
    soft = jnp.maximum(x, lax.log2(1.0 + jnp.exp2(jnp.minimum(x, 100.0))))
    below = direct * jnp.exp2(soft * rate)
    u = jnp.tanh(mix[gpoints:])
    wide = 1.0 + u
    less = GROUND - u
    gap = (0.75 * (1.0 - ASYM)) * wide
    more = less + gap
    square = less * more
    inverse = lax.rsqrt(square)
    bend = jnp.tanh(((square * inverse) * soft) * DEPTH)
    slope = bend * inverse
    total = (less + more) * slope
    r = gap * slope
    bend2 = bend * bend
    plus = 1.0 + bend2
    scattered = wide * (direct - below)
    rising = scattered * back
    falling = scattered * fall
    state_ref[2, level] = big_b
    state_ref[3, level] = big_q + direct
    z = 1.0 / ((plus + total) - r * big_b)
    h = (big_q + big_b * rising) * z
    t2 = 1.0 - bend2
    state_ref[0, level] = t2 * z
    state_ref[1, level] = r * h + rising
    return below, (r + (plus - total) * big_b) * z, t2 * h + falling


def fold(parts):
    place = lax.broadcasted_iota(jnp.int32, parts[0].shape, 0)
    distance = 1
    while len(parts) > 1:
        even = (place & distance) == 0
        parts = [
            jnp.where(even, p, q) + pltpu.roll(jnp.where(even, q, p), 8 - distance, 0)
            for p, q in zip(parts[0::2], parts[1::2])
        ]
        distance *= 2
    rest = parts[0]
    while distance < 8:
        rest = rest + pltpu.roll(rest, 8 - distance, 0)
        distance *= 2
    return rest


def gather_g(value):
    parts = [value[i : i + 8] for i in range(0, value.shape[0], 8)]
    while len(parts) > 1:
        parts = [p + q for p, q in zip(parts[0::2], parts[1::2])]
    return parts[0]


class Ascent:
    def __init__(self, albedo, lit, carry, state_ref, rise_ref):
        lev = state_ref.shape[1]
        self.state_ref, self.rise_ref, self.lit = state_ref, rise_ref, lit
        direct, big_b, big_q = carry
        self.up = (albedo[1] * big_q + albedo[0] * direct) / (1.0 - albedo[1] * big_b)
        last = fold([gather_g(big_b * self.up + big_q + direct), gather_g(self.up)])
        rise_ref[2 * lev : 2 * lev + 8, :] = last * lit
        self.parts = []

    def level(self, level):
        state_ref = self.state_ref
        self.up = state_ref[0, level] * self.up + state_ref[1, level]
        down = state_ref[2, level] * self.up + state_ref[3, level]
        self.parts = [gather_g(down), gather_g(self.up)] + self.parts
        if level % 4 == 0:
            self.rise_ref[2 * level : 2 * level + 8, :] = fold(self.parts) * self.lit
            self.parts = []


def solar_column(solar_ref):
    row = solar_ref[...]
    n = row.shape[1]
    diagonal = lax.broadcasted_iota(jnp.int32, (n, n), 0) == lax.broadcasted_iota(jnp.int32, (n, n), 1)
    return jnp.sum(jnp.where(diagonal, row, 0.0), axis=1, keepdims=True)


def flux_kernel(
    n, span, gas_hbm, cos_hbm, lit_hbm, weight_hbm, solar_hbm, area_hbm, fine_albedo_hbm, parent_hbm,
    flux_ref, big_ref, states_ref, end_ref, albedo_ref, cosf_ref, litf_ref, mine_ref, pieces_ref,
    edge_ref, halo_ref, inputs_ref, mix_ref, next_ref, gas_ref, cos_ref, lit_ref, weight_ref, solar_ref,
    area_ref, fine_albedo_ref, parent_ref, send_sem, recv_sem, edge_send, edge_recv, load_sem,
):
    ncb = cos_ref.shape[0]
    blocks = area_ref.shape[0]
    lev = gas_ref.shape[1]
    gpoints = solar_ref.shape[1]
    rows = 2 * gpoints
    slots = states_ref.shape[0]
    me = lax.axis_index("blk")
    peers = [lax.rem(me + shift, n) for shift in range(1, n)]
    mesh_id = pl.DeviceIdType.MESH

    sources = [
        (weight_hbm, weight_ref), (parent_hbm, parent_ref), (area_hbm, area_ref),
        (fine_albedo_hbm, fine_albedo_ref), (solar_hbm, solar_ref), (cos_hbm, cos_ref), (lit_hbm, lit_ref),
        (gas_hbm.at[:, :, 0:CB], gas_ref.at[:, :, 0:CB]), (gas_hbm.at[:, :, CB:], gas_ref.at[:, :, CB:]),
    ]
    loads = [pltpu.make_async_copy(src, dst, load_sem.at[i]) for i, (src, dst) in enumerate(sources)]
    for load in loads:
        load.start()
    barrier = pltpu.get_barrier_semaphore()
    for peer in peers:
        pl.semaphore_signal(barrier, inc=1, device_id={"blk": peer}, device_id_type=mesh_id)

    for load in loads[:-1]:
        load.wait()
    expand_weight(weight_ref, big_ref)
    for pair in range(2):
        stage(0, 2 * pair * CHUNK, gas_ref, inputs_ref.at[pair])
        product(inputs_ref.at[pair], big_ref, mix_ref.at[pair])
    first, second, number = local_albedo(area_ref, fine_albedo_ref, parent_ref, span)
    own_piece(first, second, number, mine_ref)
    cosf_ref[...] = cos_ref[...].astype(jnp.float32)
    litf_ref[...] = lit_ref[...].astype(jnp.float32)
    solar = solar_column(solar_ref)
    loads[-1].wait()

    def order(i):
        if isinstance(i, int):
            return i * (ncb - 1) if i < 2 else i - 1
        return jnp.where(i < 2, i * (ncb - 1), i - 1)

    def wide(row):
        return jnp.broadcast_to(row, (gpoints, CB))

    def stage_pair(cb, pair):
        stage(cb, 2 * pair * CHUNK, gas_ref, inputs_ref.at[pair])

    def down(i, mix_ref, next_ref):
        cb = order(i)
        slot = lax.rem(i, slots)
        state_ref = states_ref.at[slot]
        mu = cosf_ref[pl.ds(cb, 1), :]
        rate = wide((-TAU_SCALE) / mu)
        back = (0.5 * (0.5 * SSA_MAX)) * (1.0 - ASYM * mu)
        fall = wide(0.5 * SSA_MAX - back)
        back = wide(back)
        zero = jnp.zeros((gpoints, CB), jnp.float32)
        carry = (solar * mu, zero, zero)
        after = order(jnp.minimum(i + 1, ncb - 1))
        for pair in range(2):
            stage_pair(after, pair)
        for level in range(lev):
            for pair, place in enumerate((8, 20)):
                if level == place:
                    product(inputs_ref.at[pair], big_ref, next_ref.at[pair])
            chunk, j = level // CHUNK, level % CHUNK
            left = chunk % 2 * CB
            mix = mix_ref[chunk // 2, j * rows : (j + 1) * rows, left : left + CB]
            carry = layer(mix, rate, back, fall, carry, state_ref, level)
        for j in range(3):
            end_ref[slot, j] = carry[j]

    def up(i):
        cb = order(i)
        slot = lax.rem(i, slots)
        albedo = [albedo_ref[s, pl.ds(cb, 1), :] for s in range(2)]
        rise = Ascent(
            albedo, litf_ref[pl.ds(cb, 1), :], [end_ref[slot, j] for j in range(3)],
            states_ref.at[slot], flux_ref.at[cb + 1],
        )
        for level in reversed(range(lev)):
            rise.level(level)

    sends = [
        pltpu.make_async_remote_copy(
            src_ref=mine_ref,
            dst_ref=pieces_ref.at[i],
            send_sem=send_sem.at[i],
            recv_sem=recv_sem.at[i],
            device_id={"blk": peer},
            device_id_type=mesh_id,
        )
        for i, peer in enumerate(peers)
    ]

    def send():
        pl.semaphore_wait(barrier, n - 1)
        for copy in sends:
            copy.start()

    lower = me < n // 2

    @pl.when(jnp.logical_not(lower))
    def _():
        send()

    edges = [
        pltpu.make_async_remote_copy(
            src_ref=edge_ref.at[i],
            dst_ref=halo_ref.at[i],
            send_sem=edge_send.at[i],
            recv_sem=edge_recv.at[i],
            device_id={"blk": peer},
            device_id_type=mesh_id,
        )
        for i, peer in ((0, peers[-1]), (1, peers[0]))
    ]

    def early_up(i, unused):
        up(i)

        @pl.when(i == 1)
        def _():
            edge_ref[0] = flux_ref[1]
            edge_ref[1] = flux_ref[ncb]
            for copy in edges:
                copy.start()

        return unused

    def receive():
        for copy in sends:
            copy.wait()
        start_span = me * (ncb * CB // span)
        pieces = [mine_ref] + [pieces_ref.at[i] for i in range(n - 1)]
        direct, diffuse = pick_albedo(pieces, start_span, span, blocks, ncb)
        albedo_ref[0] = direct
        albedo_ref[1] = diffuse

    def two_steps(j, unused):
        down(2 * j, mix_ref, next_ref)

        def second(i, inner):
            down(2 * j + 1, next_ref, mix_ref)
            return inner

        lax.fori_loop(0, jnp.minimum(me + 1, 1), second, 0)

        @pl.when(jnp.logical_and(j == 0, lower))
        def _():
            send()

        @pl.when(j == 1)
        def _():
            receive()

        lax.fori_loop(jnp.where(j < 2, 0, 2 * j), jnp.where(j < 1, 0, 2 * j + 2), early_up, 0)
        return unused

    lax.fori_loop(0, ncb // 2, two_steps, 0)
    for copy in edges:
        copy.wait()
    flux_ref[0] = halo_ref[1]
    flux_ref[ncb + 1] = halo_ref[0]


def side_kernel(flux_ref, neighbours_ref, weights_ref, out_hbm, out_ref, both_ref, out_sem):
    interfaces, parts, cols = out_ref.shape
    ncb = cols // CB
    rows = flux_ref.shape[1]
    start = (lax.axis_index("grp") * lax.axis_size("blk") + lax.axis_index("blk")) * cols

    def split(block):
        value = flux_ref[block]
        high = value.astype(jnp.bfloat16).astype(jnp.float32)
        both_ref[block] = jnp.concatenate([high, value - high], axis=0).astype(jnp.bfloat16)

    place = lax.broadcasted_iota(jnp.int32, (3 * CB, CB), 0)
    split(0)
    split(1)
    copies = []
    for cb in range(ncb):
        split(cb + 2)
        own = slice(cb * CB, (cb + 1) * CB)
        picked = neighbours_ref[:, own] - (start + (cb - 1) * CB)
        weights = weights_ref[:, own]
        window = jnp.concatenate([both_ref[cb + j] for j in range(3)], axis=1)
        chosen = (place == picked[0:1]).astype(jnp.float32).astype(jnp.bfloat16)
        beside = jnp.dot(window, chosen, preferred_element_type=jnp.float32)
        centre = flux_ref[cb + 1]
        first = centre + weights[0:1] * (beside[:rows] + beside[rows:] - centre)
        results = [first[r : r + 8] for r in range(0, rows, 8)]
        for k in range(1, 3):
            row = jnp.broadcast_to(picked[k : k + 1], (8, CB))
            lanes, block = row & (CB - 1), row // CB
            share = jnp.broadcast_to(weights[k : k + 1], (8, CB))
            for i, r in enumerate(range(0, rows, 8)):
                near = [flux_ref[cb + j, r : r + 8, :] for j in range(3)]
                before, here, after = [
                    jnp.take_along_axis(v, lanes, axis=1, mode="promise_in_bounds") for v in near
                ]
                beside = jnp.where(block == 0, before, jnp.where(block == 1, here, after))
                results[i] = results[i] + share * (beside - near[1])
        for r, result in zip(range(0, rows, 8), results):
            top = r // parts
            count = min(8 // parts, interfaces - top)
            out_ref[top : top + count, :, own] = result[: count * parts].reshape(count, parts, CB)
        copy = pltpu.make_async_copy(out_ref.at[:, :, own], out_hbm.at[:, :, own], out_sem.at[cb])
        copy.start()
        copies.append(copy)
    for copy in copies:
        copy.wait()


def local(
    gas_state, cos_zenith, daylit, fine_area, fine_albedo, parent_of,
    optics_weight, solar_weight, neighbours, side_weight,
):
    n = lax.axis_size("blk")
    feats, lev, cols = gas_state.shape
    gpoints = solar_weight.shape[0]
    ncb = cols // CB
    blocks = fine_area.shape[0] // FB
    span = cols // blocks
    rows = round_up(2 * (lev + 1), 8)
    full = pl.BlockSpec(memory_space=VMEM)
    slots = 4
    fluxes = pl.pallas_call(
        functools.partial(flux_kernel, n, span),
        out_shape=jax.ShapeDtypeStruct((ncb + 2, rows, CB), jnp.float32),
        in_specs=[pl.BlockSpec(memory_space=pltpu.HBM)] * 8,
        out_specs=full,
        scratch_shapes=[
            VMEM((CHUNK * 2 * gpoints, 2 * CHUNK * feats), jnp.bfloat16),
            VMEM((slots, 4, lev, gpoints, CB), jnp.float32),
            VMEM((slots, 3, gpoints, CB), jnp.float32),
            VMEM((2, ncb, CB), jnp.float32),
            VMEM((ncb, CB), jnp.float32),
            VMEM((ncb, CB), jnp.float32),
            VMEM((2 * blocks + 16, CB), jnp.bfloat16),
            VMEM((n - 1, 2 * blocks + 16, CB), jnp.bfloat16),
            VMEM((2, rows, CB), jnp.float32),
            VMEM((2, rows, CB), jnp.float32),
            VMEM((2, CHUNK * feats, 2 * CB), gas_state.dtype),
            VMEM((2, CHUNK * 2 * gpoints, 2 * CB), jnp.float32),
            VMEM((2, CHUNK * 2 * gpoints, 2 * CB), jnp.float32),
            VMEM((feats, lev, cols), gas_state.dtype),
            VMEM((ncb, CB), cos_zenith.dtype),
            VMEM((ncb, CB), daylit.dtype),
            VMEM((feats, 2 * gpoints), optics_weight.dtype),
            VMEM((1, gpoints), jnp.float32),
            VMEM((blocks, FB), jnp.float32),
            VMEM(fine_albedo.shape, jnp.float32),
            VMEM((blocks, FB), parent_of.dtype),
            pltpu.SemaphoreType.DMA((n - 1,)),
            pltpu.SemaphoreType.DMA((n - 1,)),
            pltpu.SemaphoreType.DMA((2,)),
            pltpu.SemaphoreType.DMA((2,)),
            pltpu.SemaphoreType.DMA((9,)),
        ],
        compiler_params=pltpu.CompilerParams(
            collective_id=0, has_side_effects=True, vmem_limit_bytes=24 << 20
        ),
    )(*[
        pltpu.with_memory_space_constraint(value, pltpu.HBM)
        for value in (
            gas_state, cos_zenith.reshape(ncb, CB), daylit.reshape(ncb, CB), optics_weight.T,
            solar_weight.reshape(1, gpoints), fine_area.reshape(blocks, FB), fine_albedo,
            parent_of.reshape(blocks, FB),
        )
    ])
    result = pl.pallas_call(
        side_kernel,
        out_shape=jax.ShapeDtypeStruct((lev + 1, 2, cols), jnp.float32),
        in_specs=[full] * 3,
        out_specs=pl.BlockSpec(memory_space=pl.ANY),
        scratch_shapes=[
            VMEM((lev + 1, 2, cols), jnp.float32),
            VMEM((ncb + 2, 2 * rows, CB), jnp.bfloat16),
            pltpu.SemaphoreType.DMA((ncb,)),
        ],
        compiler_params=pltpu.CompilerParams(vmem_limit_bytes=8 << 20),
    )(fluxes, neighbours, side_weight)
    return jnp.transpose(result, (1, 0, 2))


def solution(mesh):
    columns = P(("grp", "blk"))
    last = P(None, ("grp", "blk"))
    in_specs = (
        P(None, None, ("grp", "blk")), columns, columns, columns, last, columns, P(), P(), last, last,
    )
    out_specs = P(None, None, ("grp", "blk"))
    return jax.shard_map(local, mesh=mesh, in_specs=in_specs, out_specs=out_specs, check_vma=False)
```
